32 devices in a mesh: group: 2 (over x), dev: 16 (over z, y, core).
Axes of the slice: x: 2, y: 2, z: 4, core: 2. Of those that a mesh axis runs over, the one named last changes fastest.
Arguments:
- teacher: bfloat16 [192, 8192], P(('group', 'dev')), may hold values from -6 to 6
- owner: int32 [2, 16], replicated, may hold values from 0 to 15, each once within a row
- proj_tiles: bfloat16 [8192, 4096], P('dev'), may hold values from -0.0625 to 0.0625
- student_tiles: bfloat16 [192, 4096], P(('group', 'dev')), may hold values from -6 to 6
Outputs:
- grad_proj_tiles: bfloat16 [8192, 4096], P('dev')
- grad_student_tiles: bfloat16 [192, 4096], P(('group', 'dev'))
The draws below stay inside these ranges and needn't reach their ends.
Inputs may be any that keep to these rules, and one draw needn't show every extreme that they name: Each row of owner is a permutation of 0 to 15.
All inputs are finite; a program needn't handle non-finite values.
Results may differ from the reference program's by a relative error of at most 0.0069.
Values may be sent and summed in bfloat16 or wider, within the bound.
No kernel may reach another device: no remote copies, remote signals or barrier semaphores. Data moves between devices by JAX's collectives and lax.ppermute only.
A program may use at most 64 MiB of HBM per device.

```python
import math
import jax
import jax.numpy as jnp
from jax import lax

DT = 8192
DS = 4096
TOK_DEV = 6
FEAT_SPLIT = 16
BT = 512
BS = 4096
SPAN = 6
TOKENS = 192
N_GROUP = 2
N_DEV = 16


def block_scale(stream_key, dims, split, smallest, largest):
    def one(position, shards_of):
        heights = jax.random.uniform(jax.random.fold_in(jax.random.fold_in(stream_key, 6), position), (shards_of,), jnp.float32, smallest / len(split), largest / len(split))
        return jnp.repeat(jnp.exp(heights), dims[position] // shards_of).reshape((-1,) + (1,) * (len(dims) - position - 1))

    loudness = one(*split[0])
    for cut in split[1:]:
        loudness = loudness * one(*cut)
    return loudness


def scatter_about(own_key, shape, width, limit, cuts=(), kind=jnp.bfloat16):
    array = jax.random.normal(own_key, shape, jnp.float32) * width
    if len(cuts) > 0:
        array = block_scale(own_key, shape, cuts, -0.22, 0.18) * array
    return jnp.clip(array, min=-limit, max=limit).astype(kind)


def setup_inputs(seed: int = 0) -> dict:
    splits = jax.random.split(jax.random.key(seed), 5)
    return {
        "teacher": scatter_about(splits[0], (TOKENS, DT), 1.0, 6.0, ((0, 32),)),
        "owner": jax.vmap(lambda own: jax.random.permutation(own, N_DEV))(jax.random.split(splits[1], N_GROUP)).reshape((N_GROUP, N_DEV)).astype(jnp.int32),
        "proj_tiles": scatter_about(splits[2], (N_DEV * BT, BS), DT ** -0.5, 0.0625, ((0, 16),)),
        "student_tiles": scatter_about(splits[3], (N_GROUP * N_DEV * SPAN, BS), 1.0, 6.0, ((0, 32),)),
    }


epsilon = 1e-06

def reference(teacher, owner, proj_tiles, student_tiles):
    spread = N_DEV // FEAT_SPLIT
    block_teacher = DT // FEAT_SPLIT
    block_student = DS // spread
    half_rows = N_DEV * TOK_DEV
    span_rows = half_rows // FEAT_SPLIT
    weight = proj_tiles.reshape(spread, FEAT_SPLIT, block_teacher, block_student).transpose(1, 2, 0, 3).reshape(DT, DS)
    student = student_tiles.reshape(N_GROUP, spread, FEAT_SPLIT, span_rows, block_student).transpose(0, 2, 3, 1, 4).reshape(N_GROUP, half_rows, DS)
    states = teacher.reshape(N_GROUP, half_rows, DT)
    grad_weight = jnp.zeros((DT, DS), jnp.float32)
    grad_list = []
    for half_index in range(N_GROUP):
        projected = jnp.dot(states[half_index], weight, preferred_element_type=jnp.float32)
        owner_row = owner[half_index].astype(jnp.int32)
        ordered = jnp.take(projected.reshape(N_DEV, TOK_DEV, DS), owner_row, axis=0).reshape(half_rows, DS)
        root_mean = jnp.sqrt(lax.optimization_barrier(jnp.mean(ordered * ordered, axis=1, keepdims=True)) + epsilon)
        normed = ordered / root_mean
        target = student[half_index].astype(jnp.float32)
        grad_list.append((target - normed).astype(jnp.bfloat16))
        upstream = normed - target
        inner_mean = lax.optimization_barrier(jnp.mean(upstream * normed, axis=1, keepdims=True))
        row_slope = ((upstream - normed * inner_mean) / root_mean).astype(jnp.bfloat16)
        teacher_order = jnp.zeros((N_DEV, TOK_DEV, DS), jnp.bfloat16).at[owner_row].set(row_slope.reshape(N_DEV, TOK_DEV, DS))
        grad_weight = grad_weight + lax.dot_general(states[half_index], teacher_order.reshape(half_rows, DS), (((0,), (0,)), ((), ())), preferred_element_type=jnp.float32)
    scale_factor = 1.0 / math.sqrt(N_GROUP * half_rows)
    grad_proj = (grad_weight * scale_factor).astype(jnp.bfloat16)
    grad_proj = grad_proj.reshape(FEAT_SPLIT, block_teacher, spread, block_student).transpose(2, 0, 1, 3).reshape(N_DEV * block_teacher, block_student)
    grad_student = jnp.stack(grad_list).reshape(N_GROUP, FEAT_SPLIT, span_rows, spread, block_student).transpose(0, 3, 1, 2, 4).reshape(N_GROUP * N_DEV * span_rows, block_student)
    return (grad_proj, grad_student)
```

```python
import math

import jax
import jax.numpy as jnp
from jax import lax
from jax.sharding import PartitionSpec as P

DS = 4096
FEAT_SPLIT = 16
NEAR = 4


epsilon = 1e-06


def across(value, group_mask, dev_mask):
    groups, devices = lax.axis_size("group"), lax.axis_size("dev")
    pairs = [
        (g * devices + d, (g ^ group_mask) * devices + (d ^ dev_mask))
        for g in range(groups)
        for d in range(devices)
    ]
    return lax.ppermute(value, ("group", "dev"), pairs)


def gather_wide(block, column_index, spread):
    step = 1
    while step < spread:
        arrived = across(block, 0, step * FEAT_SPLIT)
        my_bit = (column_index & step) > 0
        block = jnp.concatenate(
            [jnp.where(my_bit, arrived, block), jnp.where(my_bit, block, arrived)], axis=0
        )
        step *= 2
    return block


def shards(teacher, owner, proj_tiles, student_tiles):
    row_count, width = teacher.shape
    device_count = lax.axis_size("dev")
    spread = device_count // FEAT_SPLIT
    block_teacher = width // FEAT_SPLIT
    block_student = proj_tiles.shape[1]
    unit = spread * row_count
    far = FEAT_SPLIT // NEAR
    dev_index = lax.axis_index("dev")
    feat_index = dev_index % FEAT_SPLIT
    column_index = dev_index // FEAT_SPLIT
    group_index = lax.axis_index("group")

    full_rows = gather_wide(teacher, column_index, spread)
    pieces = full_rows.reshape(unit, FEAT_SPLIT, block_teacher).transpose(1, 0, 2)
    relative = jnp.arange(FEAT_SPLIT)
    pieces = jnp.take(pieces, feat_index ^ relative, axis=0)
    pieces = pieces.reshape(far, NEAR, unit, block_teacher)
    held = jnp.stack(
        [pieces[0]] + [across(pieces[m], 0, m * NEAR) for m in range(1, far)]
    )
    slots = jnp.stack(
        [held[:, 0]] + [across(held[:, m], 0, m) for m in range(1, NEAR)]
    )
    slots = slots.transpose(1, 0, 2, 3).reshape(device_count, row_count, block_teacher)

    place = jnp.array(
        [c | (n << 1) | (f << 2) for c in range(2) for n in range(NEAR // 2) for f in range(far)]
    )
    owner_row = lax.dynamic_index_in_dim(owner, group_index, 0, keepdims=False)
    student_block = ((feat_index ^ place)[:, None] * spread + jnp.arange(spread)[None]).reshape(-1)
    teacher_block = owner_row[student_block]
    slot = ((teacher_block % FEAT_SPLIT) ^ feat_index) * spread + teacher_block // FEAT_SPLIT
    states = jnp.take(slots, slot, axis=0).reshape(device_count * row_count, block_teacher)
    other_states = across(states, 1, 0)

    partial_value = jnp.dot(states, proj_tiles, preferred_element_type=jnp.float32)
    partial_value = partial_value.reshape(2, -1, block_student)
    for mask in (1, 2):
        arrived = across(partial_value[1].astype(jnp.bfloat16), 0, mask)
        partial_value = (partial_value[0] + arrived.astype(jnp.float32)).reshape(
            2, -1, block_student
        )
    partial_value = partial_value.reshape(far, unit, block_student)
    projected = partial_value[0]
    leaving = partial_value.astype(jnp.bfloat16)
    for m in range(1, far):
        projected = projected + across(leaving[m], 0, m * NEAR).astype(jnp.float32)

    target = student_tiles.astype(jnp.float32)
    row_sums = jnp.stack(
        [jnp.sum(projected * projected, axis=1), jnp.sum(target * projected, axis=1)]
    )
    step = 1
    while step < spread:
        row_sums = row_sums + across(row_sums, 0, step * FEAT_SPLIT)
        step *= 2
    root_mean = jnp.sqrt(row_sums[0] / DS + epsilon)
    normed = projected / root_mean[:, None]
    inner_mean = (row_sums[0] / (root_mean * root_mean) - row_sums[1] / root_mean) / DS
    upstream = normed - target
    row_slope = ((upstream - normed * inner_mean[:, None]) / root_mean[:, None]).astype(
        jnp.bfloat16
    )

    line = jnp.concatenate(
        [row_slope] + [across(row_slope, 0, m * NEAR) for m in range(1, far)], axis=0
    )
    own = [line, across(line, 0, 2)]
    other = [across(line, 1, 0), across(line, 1, 2)]
    own, other = jnp.concatenate(own), jnp.concatenate(other)
    slopes = jnp.concatenate([own, across(own, 0, 1), other, across(other, 0, 1)])
    grad_total = lax.dot_general(
        jnp.concatenate([states, other_states]),
        slopes,
        (((0,), (0,)), ((), ())),
        preferred_element_type=jnp.float32,
    )
    scale_factor = 1.0 / math.sqrt(lax.axis_size("group") * states.shape[0])
    return (
        (grad_total * scale_factor).astype(jnp.bfloat16),
        (target - normed).astype(jnp.bfloat16),
    )


def solution(mesh):
    placed = (P(("group", "dev"), None), P(), P("dev", None), P(("group", "dev"), None))
    return jax.shard_map(
        shards,
        mesh=mesh,
        in_specs=placed,
        out_specs=(P("dev", None), P(("group", "dev"), None)),
        check_vma=False,
    )
```

```python
import functools
import math

import jax
import jax.numpy as jnp
from jax import lax
from jax.experimental import pallas as pl
from jax.experimental.pallas import tpu as pltpu
from jax.sharding import PartitionSpec as P

DS = 4096
FEAT_SPLIT = 16
NEAR = 4


epsilon = 1e-06


def across(value, group_mask, dev_mask):
    groups, devices = lax.axis_size("group"), lax.axis_size("dev")
    pairs = [
        (g * devices + d, (g ^ group_mask) * devices + (d ^ dev_mask))
        for g in range(groups)
        for d in range(devices)
    ]
    return lax.ppermute(value, ("group", "dev"), pairs)


def gather_wide(block, column_index, spread):
    step = 1
    while step < spread:
        arrived = across(block, 0, step * FEAT_SPLIT)
        my_bit = (column_index & step) > 0
        block = jnp.concatenate(
            [jnp.where(my_bit, arrived, block), jnp.where(my_bit, block, arrived)], axis=0
        )
        step *= 2
    return block


def wide_shards(teacher, owner, proj_tiles, student_tiles):
    row_count, width = teacher.shape
    device_count = lax.axis_size("dev")
    spread = device_count // FEAT_SPLIT
    block_teacher = width // FEAT_SPLIT
    block_student = proj_tiles.shape[1]
    unit = spread * row_count
    far = FEAT_SPLIT // NEAR
    dev_index = lax.axis_index("dev")
    feat_index = dev_index % FEAT_SPLIT
    column_index = dev_index // FEAT_SPLIT
    group_index = lax.axis_index("group")

    full_rows = gather_wide(teacher, column_index, spread)
    pieces = full_rows.reshape(unit, FEAT_SPLIT, block_teacher).transpose(1, 0, 2)
    relative = jnp.arange(FEAT_SPLIT)
    pieces = jnp.take(pieces, feat_index ^ relative, axis=0)
    pieces = pieces.reshape(far, NEAR, unit, block_teacher)
    held = jnp.stack(
        [pieces[0]] + [across(pieces[m], 0, m * NEAR) for m in range(1, far)]
    )
    slots = jnp.stack(
        [held[:, 0]] + [across(held[:, m], 0, m) for m in range(1, NEAR)]
    )
    slots = slots.transpose(1, 0, 2, 3).reshape(device_count, row_count, block_teacher)

    place = jnp.array(
        [c | (n << 1) | (f << 2) for c in range(2) for n in range(NEAR // 2) for f in range(far)]
    )
    owner_row = lax.dynamic_index_in_dim(owner, group_index, 0, keepdims=False)
    student_block = ((feat_index ^ place)[:, None] * spread + jnp.arange(spread)[None]).reshape(-1)
    teacher_block = owner_row[student_block]
    slot = ((teacher_block % FEAT_SPLIT) ^ feat_index) * spread + teacher_block // FEAT_SPLIT
    states = jnp.take(slots, slot, axis=0).reshape(device_count * row_count, block_teacher)
    other_states = across(states, 1, 0)

    partial_value = jnp.dot(states, proj_tiles, preferred_element_type=jnp.float32)
    partial_value = partial_value.reshape(2, -1, block_student)
    for mask in (1, 2):
        arrived = across(partial_value[1].astype(jnp.bfloat16), 0, mask)
        partial_value = (partial_value[0] + arrived.astype(jnp.float32)).reshape(
            2, -1, block_student
        )
    partial_value = partial_value.reshape(far, unit, block_student)
    projected = partial_value[0]
    leaving = partial_value.astype(jnp.bfloat16)
    for m in range(1, far):
        projected = projected + across(leaving[m], 0, m * NEAR).astype(jnp.float32)

    target = student_tiles.astype(jnp.float32)
    row_sums = jnp.stack(
        [jnp.sum(projected * projected, axis=1), jnp.sum(target * projected, axis=1)]
    )
    step = 1
    while step < spread:
        row_sums = row_sums + across(row_sums, 0, step * FEAT_SPLIT)
        step *= 2
    root_mean = jnp.sqrt(row_sums[0] / DS + epsilon)
    normed = projected / root_mean[:, None]
    inner_mean = (row_sums[0] / (root_mean * root_mean) - row_sums[1] / root_mean) / DS
    upstream = normed - target
    row_slope = ((upstream - normed * inner_mean[:, None]) / root_mean[:, None]).astype(
        jnp.bfloat16
    )

    line = jnp.concatenate(
        [row_slope] + [across(row_slope, 0, m * NEAR) for m in range(1, far)], axis=0
    )
    own = [line, across(line, 0, 2)]
    other = [across(line, 1, 0), across(line, 1, 2)]
    own, other = jnp.concatenate(own), jnp.concatenate(other)
    slopes = jnp.concatenate([own, across(own, 0, 1), other, across(other, 0, 1)])
    grad_total = lax.dot_general(
        jnp.concatenate([states, other_states]),
        slopes,
        (((0,), (0,)), ((), ())),
        preferred_element_type=jnp.float32,
    )
    scale_factor = 1.0 / math.sqrt(lax.axis_size("group") * states.shape[0])
    return (
        (grad_total * scale_factor).astype(jnp.bfloat16),
        (target - normed).astype(jnp.bfloat16),
    )


LANES = 128
TILES = 2
MIB = 1 << 20


def local_call(kernel, outs, args, scratch=(), scalars=0, flops=0, moved=0, limit=8, **extra):
    in_smem = pl.BlockSpec(memory_space=pltpu.SMEM)
    in_vmem = pl.BlockSpec(memory_space=pltpu.VMEM)
    specs = [in_smem] * scalars + [in_vmem] * (len(args) - scalars)
    return pl.pallas_call(
        kernel,
        out_shape=[jax.ShapeDtypeStruct(shape, kind) for shape, kind in outs],
        in_specs=specs,
        out_specs=[in_vmem] * len(outs),
        scratch_shapes=list(scratch),
        compiler_params=pltpu.CompilerParams(vmem_limit_bytes=limit * MIB),
        cost_estimate=pl.CostEstimate(flops=flops, bytes_accessed=moved, transcendentals=0),
        **extra,
    )(*args)


def split_kernel(ids_ref, x_ref, *outs):
    part = x_ref.shape[1] // len(outs)
    for m, out in enumerate(outs):
        first = pl.multiple_of((ids_ref[2] ^ m) * part, part)
        out[...] = x_ref[:, pl.ds(first, part)]


def pack_kernel(ids_ref, *refs):
    held, outs = refs[: len(refs) // 2], refs[len(refs) // 2 :]
    for k, out in enumerate(outs):
        part = out.shape[2]
        first = pl.multiple_of((ids_ref[3] ^ k) * part, part)
        for m, source in enumerate(held):
            out[m] = source[:, pl.ds(first, part)]


def product(lhs, tiles_ref, first, leaving_ref, staying_ref):
    half, width = staying_ref.shape
    step = min(width, 512)
    for start in range(0, width, step):
        part = jnp.dot(
            lhs,
            tiles_ref[:, first + start : first + start + step],
            preferred_element_type=jnp.float32,
        )
        staying_ref[:, start : start + step] = part[:half]
        leaving_ref[:, start : start + step] = part[half:].astype(jnp.bfloat16)


def order_kernel(place, ids_ref, owner_ref, *refs):
    sources, (tiles_ref, lhs_ref, leaving_ref, staying_ref, slots, rows) = refs[:-6], refs[-6:]
    far, unit = sources[0].shape[0], sources[0].shape[1]
    for k, source in enumerate(sources):
        for m in range(far):
            slots[m * len(sources) + k] = source[m].astype(jnp.float32)
    for p, shift in enumerate(place):
        slot = owner_ref[ids_ref[1], ids_ref[0] ^ shift] ^ ids_ref[0]
        rows[p * unit : (p + 1) * unit, :] = slots[slot]
    lhs = rows[...].astype(jnp.bfloat16)
    lhs_ref[...] = lhs
    product(lhs, tiles_ref, 0, leaving_ref, staying_ref)


def rest_kernel(first, lhs_ref, tiles_ref, leaving_ref, staying_ref):
    product(lhs_ref[...], tiles_ref, first, leaving_ref, staying_ref)


def halve_kernel(kept_ref, arrived_ref, leaving_ref, staying_ref):
    half = staying_ref.shape[0]
    staying_ref[...] = kept_ref[:half] + arrived_ref[:half].astype(jnp.float32)
    leaving_ref[...] = (kept_ref[half:] + arrived_ref[half:].astype(jnp.float32)).astype(
        jnp.bfloat16
    )


def units_kernel(kept_ref, arrived_ref, own_ref, *refs):
    leaving, lines = refs[:-1], refs[-1]
    count, width = kept_ref.shape
    depth = width // LANES
    size = own_ref.shape[0]
    for t in range(depth):
        cols = slice(t * LANES, (t + 1) * LANES)
        total = kept_ref[:, cols] + arrived_ref[:, cols].astype(jnp.float32)
        lines[pl.ds(t, count, stride=depth), :] = total
    own_ref[...] = lines[:size]
    for m, out in enumerate(leaving):
        out[...] = lines[(m + 1) * size : (m + 2) * size].astype(jnp.bfloat16)


def slope_kernel(unit, *refs):
    chunks = TILES
    inputs, slopes, grads = refs[: -2 * chunks], refs[-2 * chunks : -chunks], refs[-chunks:]
    per = len(inputs) // chunks
    totals, targets = [], []
    for chunk in range(chunks):
        own, *arrived, target = inputs[chunk * per : (chunk + 1) * per]
        total = own[...]
        for other in arrived:
            total = total + other[...].astype(jnp.float32)
        totals.append(total.reshape(unit, -1, LANES))
        targets.append(target[...].astype(jnp.float32).reshape(unit, -1, LANES))

    def row_sum(parts):
        whole = sum(jnp.sum(part, axis=1, keepdims=True) for part in parts)
        return jnp.sum(whole, axis=2, keepdims=True)

    squares = row_sum([total * total for total in totals])
    products = row_sum([total * target for total, target in zip(totals, targets)])
    root_mean = jnp.sqrt(squares / DS + epsilon)
    inner_mean = (squares / (root_mean * root_mean) - products / root_mean) / DS
    for total, target, slope, grad in zip(totals, targets, slopes, grads):
        normed = total / root_mean
        upstream = normed - target
        value = (upstream - normed * inner_mean) / root_mean
        slope[...] = value.reshape(-1, LANES).astype(jnp.bfloat16)
        grad[...] = (target - normed).reshape(-1, LANES).astype(jnp.bfloat16)


def line_kernel(*refs):
    units, (out, lines) = refs[:-2], refs[-2:]
    size = units[0].shape[0]
    count, width = out.shape
    depth = width // LANES
    for m, source in enumerate(units):
        lines[m * size : (m + 1) * size, :] = source[...].astype(jnp.float32)
    for t in range(depth):
        out[:, t * LANES : (t + 1) * LANES] = lines[pl.ds(t, count, stride=depth), :].astype(
            jnp.bfloat16
        )


def grad_kernel(scale, first, step, pieces, *refs):
    own_ref, other_ref = refs[:2]
    slopes = refs[2 : 2 + pieces]
    out_ref, lhs, rhs, staged, sems = refs[-5:]
    half, width = own_ref.shape[0], slopes[0].shape[1]
    lhs[:half] = own_ref[...]
    lhs[half:] = other_ref[...]
    count = slopes[0].shape[0]
    for i, piece in enumerate(slopes):
        rhs[i * count : (i + 1) * count, :] = piece[...]
    copies = []
    for j in range(width // step):
        cols = slice(j * step, (j + 1) * step)
        part = lax.dot_general(
            lhs[...], rhs[:, cols], (((0,), (0,)), ((), ())), preferred_element_type=jnp.float32
        )
        staged[j] = (part * scale).astype(jnp.bfloat16)
        copy = pltpu.make_async_copy(
            staged.at[j], out_ref.at[:, pl.ds(first + j * step, step)], sems.at[j]
        )
        copy.start()
        copies.append(copy)
    for copy in copies:
        copy.wait()


def grad_call(scale, first, states, other_states, slopes, shape, before):
    half, block_teacher = states.shape
    width = slopes[0].shape[1]
    step = min(width, 512)
    args = [states, other_states, *slopes]
    specs = [pl.BlockSpec(memory_space=pltpu.VMEM)] * len(args)
    extra = {}
    if before is not None:
        args.append(before)
        specs.append(pl.BlockSpec(memory_space=pl.ANY))
        extra["input_output_aliases"] = {len(args) - 1: 0}
    return pl.pallas_call(
        functools.partial(grad_kernel, scale, first, step, len(slopes)),
        out_shape=jax.ShapeDtypeStruct(shape, jnp.bfloat16),
        in_specs=specs,
        out_specs=pl.BlockSpec(memory_space=pl.ANY),
        scratch_shapes=[
            pltpu.VMEM((2 * half, block_teacher), jnp.bfloat16),
            pltpu.VMEM((2 * half, width), jnp.bfloat16),
            pltpu.VMEM((width // step, block_teacher, step), jnp.bfloat16),
            pltpu.SemaphoreType.DMA((width // step,)),
        ],
        compiler_params=pltpu.CompilerParams(vmem_limit_bytes=16 * MIB),
        cost_estimate=pl.CostEstimate(
            flops=4 * half * block_teacher * width,
            bytes_accessed=2 * block_teacher * width,
            transcendentals=0,
        ),
        **extra,
    )(*args)


def line_shards(teacher, owner, proj_tiles, student_tiles):
    unit, width = teacher.shape
    block_teacher, block_student = proj_tiles.shape
    near, far = NEAR, FEAT_SPLIT // NEAR
    half = FEAT_SPLIT * unit
    cut = block_student // TILES
    depth = cut // LANES
    bf16, f32 = jnp.bfloat16, jnp.float32
    dev_index = lax.axis_index("dev")
    ids = jnp.stack([dev_index, lax.axis_index("group"), dev_index // near, dev_index % near])

    held = local_call(
        split_kernel, [((unit, width // far), bf16)] * far, [ids, teacher], scalars=1
    )
    held = [held[0]] + [across(held[m], 0, m * near) for m in range(1, far)]
    packed = local_call(
        pack_kernel, [((far, unit, block_teacher), bf16)] * near, [ids, *held], scalars=1
    )
    slots = [packed[0]] + [across(packed[k], 0, k) for k in range(1, near)]

    place = [c | (n << 1) | (f << 2) for c in range(2) for n in range(near // 2) for f in range(far)]
    halves = [((half // 2, cut), bf16), ((half // 2, cut), f32)]
    flops = 2 * half * block_teacher * cut
    states, leaving, staying = local_call(
        functools.partial(order_kernel, place),
        [((half, block_teacher), bf16), *halves],
        [ids, owner, *slots, proj_tiles],
        scratch=[
            pltpu.VMEM((FEAT_SPLIT, unit, block_teacher), f32),
            pltpu.VMEM((half, block_teacher), f32),
        ],
        scalars=2,
        flops=flops,
    )
    parts = [(leaving, staying)]
    for chunk in range(1, TILES):
        parts.append(
            local_call(
                functools.partial(rest_kernel, chunk * cut), halves, [states, proj_tiles], flops=flops
            )
        )
    other_states = across(states, 1, 0)

    target = student_tiles.reshape(unit, TILES, depth * LANES)
    inputs = []
    size = unit * depth
    for chunk, (leaving, staying) in enumerate(parts):
        arrived = across(leaving, 0, 1)
        leaving, staying = local_call(
            halve_kernel,
            [((half // 4, cut), bf16), ((half // 4, cut), f32)],
            [staying, arrived],
        )
        arrived = across(leaving, 0, 2)
        own, *leaving = local_call(
            units_kernel,
            [((size, LANES), f32)] + [((size, LANES), bf16)] * (far - 1),
            [staying, arrived],
            scratch=[pltpu.VMEM((far * size, LANES), f32)],
        )
        inputs += [own] + [across(leaving[m - 1], 0, m * near) for m in range(1, far)]
        inputs.append(target[:, chunk].reshape(size, LANES))
    results = local_call(
        functools.partial(slope_kernel, unit), [((size, LANES), bf16)] * (2 * TILES), inputs
    )
    slopes, grads = results[:TILES], results[TILES:]

    scale = 1.0 / math.sqrt(lax.axis_size("group") * half)
    grad_proj = None
    for chunk, slope in enumerate(slopes):
        line = [slope] + [across(slope, 0, m * near) for m in range(1, far)]
        (line,) = local_call(
            line_kernel,
            [((far * unit, cut), bf16)],
            line,
            scratch=[pltpu.VMEM((far * size, LANES), f32)],
        )
        by_group, by_near = across(line, 1, 0), across(line, 0, 2)
        both = across(by_group, 0, 2) if chunk % 2 == 0 else across(by_near, 1, 0)
        own, other = [line, by_near], [by_group, both]
        pieces = (
            own
            + [across(piece, 0, 1) for piece in own]
            + other
            + [across(piece, 0, 1) for piece in other]
        )
        grad_proj = grad_call(
            scale,
            chunk * cut,
            states,
            other_states,
            pieces,
            (block_teacher, block_student),
            grad_proj,
        )
    grad_student = jnp.stack([grad.reshape(unit, cut) for grad in grads], axis=1)
    return grad_proj, grad_student.reshape(unit, block_student)


def shards(*blocks):
    if lax.axis_size("dev") == FEAT_SPLIT:
        return line_shards(*blocks)
    return wide_shards(*blocks)


def solution(mesh):
    placed = (P(("group", "dev"), None), P(), P("dev", None), P(("group", "dev"), None))
    return jax.shard_map(
        shards,
        mesh=mesh,
        in_specs=placed,
        out_specs=(P("dev", None), P(("group", "dev"), None)),
        check_vma=False,
    )
```

```python
import functools
import math

import jax
import jax.numpy as jnp
from jax import lax
from jax.experimental import pallas as pl
from jax.experimental.pallas import tpu as pltpu
from jax.sharding import PartitionSpec as P


DS = 4096
FEAT_SPLIT = 16
NEAR = 4


epsilon = 1e-06


def across(value, group_mask, dev_mask):
    groups, devices = lax.axis_size("group"), lax.axis_size("dev")
    pairs = [
        (g * devices + d, (g ^ group_mask) * devices + (d ^ dev_mask))
        for g in range(groups)
        for d in range(devices)
    ]
    return lax.ppermute(value, ("group", "dev"), pairs)


def gather_wide(block, column_index, spread):
    step = 1
    while step < spread:
        arrived = across(block, 0, step * FEAT_SPLIT)
        my_bit = (column_index & step) > 0
        block = jnp.concatenate(
            [jnp.where(my_bit, arrived, block), jnp.where(my_bit, block, arrived)], axis=0
        )
        step *= 2
    return block


def wide_shards(teacher, owner, proj_tiles, student_tiles):
    row_count, width = teacher.shape
    device_count = lax.axis_size("dev")
    spread = device_count // FEAT_SPLIT
    block_teacher = width // FEAT_SPLIT
    block_student = proj_tiles.shape[1]
    unit = spread * row_count
    far = FEAT_SPLIT // NEAR
    dev_index = lax.axis_index("dev")
    feat_index = dev_index % FEAT_SPLIT
    column_index = dev_index // FEAT_SPLIT
    group_index = lax.axis_index("group")

    full_rows = gather_wide(teacher, column_index, spread)
    pieces = full_rows.reshape(unit, FEAT_SPLIT, block_teacher).transpose(1, 0, 2)
    relative = jnp.arange(FEAT_SPLIT)
    pieces = jnp.take(pieces, feat_index ^ relative, axis=0)
    pieces = pieces.reshape(far, NEAR, unit, block_teacher)
    held = jnp.stack(
        [pieces[0]] + [across(pieces[m], 0, m * NEAR) for m in range(1, far)]
    )
    slots = jnp.stack(
        [held[:, 0]] + [across(held[:, m], 0, m) for m in range(1, NEAR)]
    )
    slots = slots.transpose(1, 0, 2, 3).reshape(device_count, row_count, block_teacher)

    place = jnp.array(
        [c | (n << 1) | (f << 2) for c in range(2) for n in range(NEAR // 2) for f in range(far)]
    )
    owner_row = lax.dynamic_index_in_dim(owner, group_index, 0, keepdims=False)
    student_block = ((feat_index ^ place)[:, None] * spread + jnp.arange(spread)[None]).reshape(-1)
    teacher_block = owner_row[student_block]
    slot = ((teacher_block % FEAT_SPLIT) ^ feat_index) * spread + teacher_block // FEAT_SPLIT
    states = jnp.take(slots, slot, axis=0).reshape(device_count * row_count, block_teacher)
    other_states = across(states, 1, 0)

    partial_value = jnp.dot(states, proj_tiles, preferred_element_type=jnp.float32)
    partial_value = partial_value.reshape(2, -1, block_student)
    for mask in (1, 2):
        arrived = across(partial_value[1].astype(jnp.bfloat16), 0, mask)
        partial_value = (partial_value[0] + arrived.astype(jnp.float32)).reshape(
            2, -1, block_student
        )
    partial_value = partial_value.reshape(far, unit, block_student)
    projected = partial_value[0]
    leaving = partial_value.astype(jnp.bfloat16)
    for m in range(1, far):
        projected = projected + across(leaving[m], 0, m * NEAR).astype(jnp.float32)

    target = student_tiles.astype(jnp.float32)
    row_sums = jnp.stack(
        [jnp.sum(projected * projected, axis=1), jnp.sum(target * projected, axis=1)]
    )
    step = 1
    while step < spread:
        row_sums = row_sums + across(row_sums, 0, step * FEAT_SPLIT)
        step *= 2
    root_mean = jnp.sqrt(row_sums[0] / DS + epsilon)
    normed = projected / root_mean[:, None]
    inner_mean = (row_sums[0] / (root_mean * root_mean) - row_sums[1] / root_mean) / DS
    upstream = normed - target
    row_slope = ((upstream - normed * inner_mean[:, None]) / root_mean[:, None]).astype(
        jnp.bfloat16
    )

    line = jnp.concatenate(
        [row_slope] + [across(row_slope, 0, m * NEAR) for m in range(1, far)], axis=0
    )
    own = [line, across(line, 0, 2)]
    other = [across(line, 1, 0), across(line, 1, 2)]
    own, other = jnp.concatenate(own), jnp.concatenate(other)
    slopes = jnp.concatenate([own, across(own, 0, 1), other, across(other, 0, 1)])
    grad_total = lax.dot_general(
        jnp.concatenate([states, other_states]),
        slopes,
        (((0,), (0,)), ((), ())),
        preferred_element_type=jnp.float32,
    )
    scale_factor = 1.0 / math.sqrt(lax.axis_size("group") * states.shape[0])
    return (
        (grad_total * scale_factor).astype(jnp.bfloat16),
        (target - normed).astype(jnp.bfloat16),
    )


LANES = 128
PARTS = (1, 1)
MIB = 1 << 20
IN_VMEM = pl.BlockSpec(memory_space=pltpu.VMEM)
IN_SMEM = pl.BlockSpec(memory_space=pltpu.SMEM)
ANYWHERE = pl.BlockSpec(memory_space=pl.ANY)
IN_HBM = pl.BlockSpec(memory_space=pltpu.HBM)


def local_call(kernel, outs, args, specs=None, scratch=(), flops=0, moved=0, limit=8, **extra):
    return pl.pallas_call(
        kernel,
        out_shape=[jax.ShapeDtypeStruct(shape, kind) for shape, kind in outs],
        in_specs=specs or [IN_VMEM] * len(args),
        out_specs=[IN_VMEM] * len(outs),
        scratch_shapes=list(scratch),
        compiler_params=pltpu.CompilerParams(vmem_limit_bytes=limit * MIB),
        cost_estimate=pl.CostEstimate(flops=flops, bytes_accessed=moved, transcendentals=0),
        **extra,
    )(*args)


def split_kernel(x_ref, near_ref, side_ref, core_ref, sems):
    far, _, part = near_ref.shape
    feat = lax.axis_index("dev")
    copies = []
    for c in range(2):
        for n in range(2):
            for m in range(far):
                out = core_ref.at[n, m] if c else (side_ref if n else near_ref).at[m]
                first = pl.multiple_of((feat ^ (c | (n << 1) | (m << 2))) * part, part)
                copies.append(
                    pltpu.make_async_copy(x_ref.at[:, pl.ds(first, part)], out, sems.at[len(copies)])
                )
    for copy in copies:
        copy.start()
    for copy in copies:
        copy.wait()


def side_kernel(side_ref, core_ref, out_ref):
    out_ref[0] = side_ref[...]
    out_ref[1] = core_ref[1]


def far_kernel(near_ref, core_ref, side_ref, *outs):
    for m, out in enumerate(outs):
        out[0] = near_ref[m]
        out[1] = core_ref[0, m]
        out[2] = side_ref[0, m]
        out[3] = side_ref[1, m]


def fetch(tiles_ref, out_ref, sems, first):
    count = sems.shape[0]
    rows, width = out_ref.shape[0] // count, out_ref.shape[1]
    copies = []
    for i in range(count):
        part = pl.ds(i * rows, rows)
        copies.append(
            pltpu.make_async_copy(
                tiles_ref.at[part, pl.ds(first, width)], out_ref.at[part], sems.at[i]
            )
        )
        copies[-1].start()
    return copies


def first_kernel(place, unit, owner_ref, tiles_ref, pick_ref, out_ref, owner_here, sem, sems):
    order = pltpu.make_async_copy(owner_ref, owner_here, sem)
    order.start()
    copies = fetch(tiles_ref, out_ref, sems, 0)
    feat, group = lax.axis_index("dev"), lax.axis_index("group")
    row = lax.broadcasted_iota(jnp.int32, pick_ref.shape, 0)
    source = lax.broadcasted_iota(jnp.int32, pick_ref.shape, 1)
    wanted = row
    order.wait()
    for p, shift in enumerate(place):
        slot = owner_here[group, feat ^ shift] ^ feat
        wanted = jnp.where(row // unit == p, row + (slot - p) * unit, wanted)
    pick_ref[...] = jnp.where(source == wanted, 1.0, 0.0).astype(jnp.bfloat16)
    for copy in copies:
        copy.wait()


def second_kernel(first, tiles_ref, out_ref, sems):
    for copy in fetch(tiles_ref, out_ref, sems, first):
        copy.wait()


def order_kernel(pick_ref, *refs):
    sources, (first_ref, second_ref) = refs[:-6], refs[-6:-4]
    lhs_ref, leaving_ref, staying_ref, slots = refs[-4:]
    near, unit = sources[0].shape[0], sources[0].shape[1]
    for m, source in enumerate(sources):
        for k in range(near):
            first = (m * near + k) * unit
            slots[first : first + unit, :] = source[k].astype(jnp.float32)
    rows = jnp.dot(
        pick_ref[...], slots[...].astype(jnp.bfloat16), preferred_element_type=jnp.float32
    )
    lhs = rows.astype(jnp.bfloat16)
    lhs_ref[...] = lhs
    half, base = staying_ref.shape[0], 0
    for tiles_ref in (first_ref, second_ref):
        width = tiles_ref.shape[1]
        step = min(width, 512)
        for start in range(0, width, step):
            tiles = tiles_ref[:, start : start + step]
            part = jnp.dot(lhs, tiles, preferred_element_type=jnp.float32)
            cols = slice(base + start, base + start + step)
            staying_ref[:, cols] = part[:half]
            leaving_ref[:, cols] = part[half:].astype(jnp.bfloat16)
        base += width


def halve_kernel(kept_ref, arrived_ref, leaving_ref, staying_ref):
    half = staying_ref.shape[0]
    staying_ref[...] = kept_ref[:half] + arrived_ref[:half].astype(jnp.float32)
    leaving_ref[...] = (kept_ref[half:] + arrived_ref[half:].astype(jnp.float32)).astype(
        jnp.bfloat16
    )


def units_kernel(kept_ref, arrived_ref, own_ref, *refs):
    leaving, lines = refs[:-1], refs[-1]
    count, width = kept_ref.shape
    depth = width // LANES
    size = own_ref.shape[0]
    for t in range(depth):
        cols = slice(t * LANES, (t + 1) * LANES)
        total = kept_ref[:, cols] + arrived_ref[:, cols].astype(jnp.float32)
        lines[pl.ds(t, count, stride=depth), :] = total
    own_ref[...] = lines[:size]
    for m, out in enumerate(leaving):
        out[...] = lines[(m + 1) * size : (m + 2) * size].astype(jnp.bfloat16)


def slope_kernel(unit, own_ref, *refs):
    arrived, (target_ref, slope_ref, grad_ref) = refs[:-3], refs[-3:]
    total = own_ref[...]
    for other in arrived:
        total = total + other[...].astype(jnp.float32)
    total = total.reshape(unit, -1, LANES)
    target = target_ref[...].astype(jnp.float32).reshape(unit, -1, LANES)

    def row_sum(part):
        return jnp.sum(jnp.sum(part, axis=1, keepdims=True), axis=2, keepdims=True)

    squares, products = row_sum(total * total), row_sum(total * target)
    root_mean = jnp.sqrt(squares / DS + epsilon)
    inner_mean = (squares / (root_mean * root_mean) - products / root_mean) / DS
    normed = total / root_mean
    upstream = normed - target
    value = (upstream - normed * inner_mean) / root_mean
    slope_ref[...] = value.reshape(-1, LANES).astype(jnp.bfloat16)
    grad_ref[...] = (target - normed).reshape(-1, LANES)


def rows_kernel(lines_ref, out_ref):
    count = out_ref.shape[0]
    depth = lines_ref.shape[0] // count
    for t in range(depth):
        cols = slice(t * LANES, (t + 1) * LANES)
        out_ref[:, cols] = lines_ref[pl.ds(t, count, stride=depth), :].astype(jnp.bfloat16)


def line_kernel(units, *refs):
    sources, outs, lines = refs[:units], refs[units:-1], refs[-1]
    size = sources[0].shape[0]
    count = outs[0].shape[0]
    depth = lines.shape[0] // count
    for m, source in enumerate(sources):
        lines[m * size : (m + 1) * size, :] = source[...].astype(jnp.float32)
    places = [(out, t) for out in outs for t in range(out.shape[1] // LANES)]
    for source, (out, t) in enumerate(places):
        cols = slice(t * LANES, (t + 1) * LANES)
        out[:, cols] = lines[pl.ds(source, count, stride=depth), :].astype(jnp.bfloat16)


def turn_kernel(own_ref, other_ref, out_ref):
    half = own_ref.shape[0]
    for i, source in enumerate((own_ref, other_ref)):
        out_ref[:, i * half : (i + 1) * half] = source[...].astype(jnp.float32).T.astype(
            jnp.bfloat16
        )


def grad_kernel(scale, step, per, states_ref, *refs):
    slopes, (out_ref, rhs, staged, sems) = refs[:-4], refs[-4:]
    copies, first = [], 0
    for chunk in range(len(slopes) // per):
        pieces = slopes[chunk * per : (chunk + 1) * per]
        count, width = pieces[0].shape
        for start in range(0, width, step):
            j = first // step
            for i, piece in enumerate(pieces):
                rhs[j % 2, i * count : (i + 1) * count, :] = piece[:, start : start + step]
            part = jnp.dot(states_ref[...], rhs[j % 2], preferred_element_type=jnp.float32)
            staged[j] = (part * scale).astype(jnp.bfloat16)
            copies.append(
                pltpu.make_async_copy(staged.at[j], out_ref.at[:, pl.ds(first, step)], sems.at[j])
            )
            copies[-1].start()
            first += step
    for copy in copies:
        copy.wait()


def grad_call(scale, states, slopes, per, shape, step=256):
    block_teacher, rows = states.shape
    count = shape[1] // step
    return pl.pallas_call(
        functools.partial(grad_kernel, scale, step, per),
        out_shape=jax.ShapeDtypeStruct(shape, jnp.bfloat16),
        in_specs=[IN_VMEM] * (len(slopes) + 1),
        out_specs=ANYWHERE,
        scratch_shapes=[
            pltpu.VMEM((2, rows, step), jnp.bfloat16),
            pltpu.VMEM((count, block_teacher, step), jnp.bfloat16),
            pltpu.SemaphoreType.DMA((count,)),
        ],
        compiler_params=pltpu.CompilerParams(vmem_limit_bytes=16 * MIB),
        cost_estimate=pl.CostEstimate(
            flops=2 * rows * block_teacher * shape[1],
            bytes_accessed=2 * block_teacher * shape[1],
            transcendentals=0,
        ),
    )(states, *slopes)


def far_across(values):
    arrived = []
    for m in range(1, len(values)):
        arrived.append(across(values[m], 0, m * NEAR))
    return arrived


def line_shards(teacher, owner, proj_tiles, student_tiles):
    unit, _ = teacher.shape
    block_teacher, block_student = proj_tiles.shape
    near, far = NEAR, FEAT_SPLIT // NEAR
    half = FEAT_SPLIT * unit
    cuts = [block_student * part // sum(PARTS) for part in PARTS]
    depth = block_student // LANES
    size = unit * depth
    bf16, f32 = jnp.bfloat16, jnp.float32

    place = [c | (n << 1) | (m << 2) for c in range(2) for n in range(2) for m in range(far)]

    block = (unit, block_teacher)
    own_near, own_side, leaving = local_call(
        split_kernel,
        [((far, *block), bf16), ((far, *block), bf16), ((2, far, *block), bf16)],
        [pltpu.with_memory_space_constraint(teacher, pltpu.HBM)],
        specs=[IN_HBM],
        scratch=[pltpu.SemaphoreType.DMA((FEAT_SPLIT,))],
    )
    core = across(leaving, 0, 1)
    (leaving,) = local_call(side_kernel, [((2, far, *block), bf16)], [own_side, core])
    side = across(leaving, 0, 2)
    held = local_call(far_kernel, [((near, *block), bf16)] * far, [own_near, core, side])
    held = [held[0]] + far_across(held)

    tiles = pltpu.with_memory_space_constraint(proj_tiles, pltpu.HBM)
    part = (block_teacher, block_student // 2)
    work = dict(flops=block_teacher * half * block_student, moved=block_teacher * block_student)
    pick, first_tiles = local_call(
        functools.partial(first_kernel, place, unit),
        [((half, half), bf16), (part, bf16)],
        [pltpu.with_memory_space_constraint(owner, pltpu.HBM), tiles],
        specs=[IN_HBM] * 2,
        scratch=[
            pltpu.SMEM(owner.shape, owner.dtype),
            pltpu.SemaphoreType.DMA,
            pltpu.SemaphoreType.DMA((8,)),
        ],
        **work,
    )
    (second_tiles,) = local_call(
        functools.partial(second_kernel, part[1]),
        [(part, bf16)],
        [tiles],
        specs=[IN_HBM],
        scratch=[pltpu.SemaphoreType.DMA((8,))],
        **work,
    )
    states, leaving, staying = local_call(
        order_kernel,
        [
            ((half, block_teacher), bf16),
            ((half // 2, block_student), bf16),
            ((half // 2, block_student), f32),
        ],
        [pick, *held, first_tiles, second_tiles],
        scratch=[pltpu.VMEM((half, block_teacher), f32)],
        flops=2 * half * block_teacher * block_student,
    )

    arrived = across(leaving, 0, 1)
    leaving, staying = local_call(
        halve_kernel,
        [((half // 4, block_student), bf16), ((half // 4, block_student), f32)],
        [staying, arrived],
    )
    states_too, leaving = lax.optimization_barrier((states, leaving))
    arrived, other_states = lax.optimization_barrier(
        (across(leaving, 0, 2), across(states_too, 1, 0))
    )
    own, *leaving = local_call(
        units_kernel,
        [((size, LANES), f32)] + [((size, LANES), bf16)] * (far - 1),
        [staying, arrived],
        scratch=[pltpu.VMEM((far * size, LANES), f32)],
    )
    arrived = far_across([None, *leaving])
    slope, grad = local_call(
        functools.partial(slope_kernel, unit),
        [((size, LANES), bf16), ((size, LANES), f32)],
        [own, *arrived, student_tiles.reshape(size, LANES)],
    )
    (grad,) = local_call(rows_kernel, [((unit, block_student), bf16)], [grad])

    line = [slope] + far_across([slope] * far)
    lines = local_call(
        functools.partial(line_kernel, far),
        [((far * unit, cut), bf16) for cut in cuts],
        line,
        scratch=[pltpu.VMEM((far * size, LANES), f32)],
    )
    scale = 1.0 / math.sqrt(lax.axis_size("group") * half)
    first, second = lines
    first_group, second_near = across(first, 1, 0), across(second, 0, 2)
    second_group, first_near = across(second, 1, 0), across(first, 0, 2)
    first_both, second_both = across(first_group, 0, 2), across(second_near, 1, 0)
    (turned,) = local_call(turn_kernel, [((block_teacher, 2 * half), bf16)], [states, other_states])
    pieces = []
    for own, other in (
        ((first, first_near), (first_group, first_both)),
        ((second, second_near), (second_group, second_both)),
    ):
        pieces += [*own, *[across(piece, 0, 1) for piece in own]]
        pieces += [*other, *[across(piece, 0, 1) for piece in other]]
    grad_proj = grad_call(scale, turned, pieces, len(pieces) // 2, (block_teacher, block_student))
    return grad_proj, grad


def shards(*blocks):
    if lax.axis_size("dev") == FEAT_SPLIT:
        return line_shards(*blocks)
    return wide_shards(*blocks)


def solution(mesh):
    placed = (P(("group", "dev"), None), P(), P("dev", None), P(("group", "dev"), None))
    return jax.shard_map(
        shards,
        mesh=mesh,
        in_specs=placed,
        out_specs=(P("dev", None), P(("group", "dev"), None)),
        check_vma=False,
    )
```

```python
import functools
import math

import jax
import jax.numpy as jnp
from jax import lax
from jax.experimental import pallas as pl
from jax.experimental.pallas import tpu as pltpu
from jax.sharding import PartitionSpec as P


DS = 4096
FEAT_SPLIT = 16
NEAR = 4


epsilon = 1e-06


def across(value, group_mask, dev_mask):
    groups, devices = lax.axis_size("group"), lax.axis_size("dev")
    pairs = [
        (g * devices + d, (g ^ group_mask) * devices + (d ^ dev_mask))
        for g in range(groups)
        for d in range(devices)
    ]
    return lax.ppermute(value, ("group", "dev"), pairs)


def gather_wide(block, column_index, spread):
    step = 1
    while step < spread:
        arrived = across(block, 0, step * FEAT_SPLIT)
        my_bit = (column_index & step) > 0
        block = jnp.concatenate(
            [jnp.where(my_bit, arrived, block), jnp.where(my_bit, block, arrived)], axis=0
        )
        step *= 2
    return block


def wide_shards(teacher, owner, proj_tiles, student_tiles):
    row_count, width = teacher.shape
    device_count = lax.axis_size("dev")
    spread = device_count // FEAT_SPLIT
    block_teacher = width // FEAT_SPLIT
    block_student = proj_tiles.shape[1]
    unit = spread * row_count
    far = FEAT_SPLIT // NEAR
    dev_index = lax.axis_index("dev")
    feat_index = dev_index % FEAT_SPLIT
    column_index = dev_index // FEAT_SPLIT
    group_index = lax.axis_index("group")

    full_rows = gather_wide(teacher, column_index, spread)
    pieces = full_rows.reshape(unit, FEAT_SPLIT, block_teacher).transpose(1, 0, 2)
    relative = jnp.arange(FEAT_SPLIT)
    pieces = jnp.take(pieces, feat_index ^ relative, axis=0)
    pieces = pieces.reshape(far, NEAR, unit, block_teacher)
    held = jnp.stack(
        [pieces[0]] + [across(pieces[m], 0, m * NEAR) for m in range(1, far)]
    )
    slots = jnp.stack(
        [held[:, 0]] + [across(held[:, m], 0, m) for m in range(1, NEAR)]
    )
    slots = slots.transpose(1, 0, 2, 3).reshape(device_count, row_count, block_teacher)

    place = jnp.array(
        [c | (n << 1) | (f << 2) for c in range(2) for n in range(NEAR // 2) for f in range(far)]
    )
    owner_row = lax.dynamic_index_in_dim(owner, group_index, 0, keepdims=False)
    student_block = ((feat_index ^ place)[:, None] * spread + jnp.arange(spread)[None]).reshape(-1)
    teacher_block = owner_row[student_block]
    slot = ((teacher_block % FEAT_SPLIT) ^ feat_index) * spread + teacher_block // FEAT_SPLIT
    states = jnp.take(slots, slot, axis=0).reshape(device_count * row_count, block_teacher)
    other_states = across(states, 1, 0)

    partial_value = jnp.dot(states, proj_tiles, preferred_element_type=jnp.float32)
    partial_value = partial_value.reshape(2, -1, block_student)
    for mask in (1, 2):
        arrived = across(partial_value[1].astype(jnp.bfloat16), 0, mask)
        partial_value = (partial_value[0] + arrived.astype(jnp.float32)).reshape(
            2, -1, block_student
        )
    partial_value = partial_value.reshape(far, unit, block_student)
    projected = partial_value[0]
    leaving = partial_value.astype(jnp.bfloat16)
    for m in range(1, far):
        projected = projected + across(leaving[m], 0, m * NEAR).astype(jnp.float32)

    target = student_tiles.astype(jnp.float32)
    row_sums = jnp.stack(
        [jnp.sum(projected * projected, axis=1), jnp.sum(target * projected, axis=1)]
    )
    step = 1
    while step < spread:
        row_sums = row_sums + across(row_sums, 0, step * FEAT_SPLIT)
        step *= 2
    root_mean = jnp.sqrt(row_sums[0] / DS + epsilon)
    normed = projected / root_mean[:, None]
    inner_mean = (row_sums[0] / (root_mean * root_mean) - row_sums[1] / root_mean) / DS
    upstream = normed - target
    row_slope = ((upstream - normed * inner_mean[:, None]) / root_mean[:, None]).astype(
        jnp.bfloat16
    )

    line = jnp.concatenate(
        [row_slope] + [across(row_slope, 0, m * NEAR) for m in range(1, far)], axis=0
    )
    own = [line, across(line, 0, 2)]
    other = [across(line, 1, 0), across(line, 1, 2)]
    own, other = jnp.concatenate(own), jnp.concatenate(other)
    slopes = jnp.concatenate([own, across(own, 0, 1), other, across(other, 0, 1)])
    grad_total = lax.dot_general(
        jnp.concatenate([states, other_states]),
        slopes,
        (((0,), (0,)), ((), ())),
        preferred_element_type=jnp.float32,
    )
    scale_factor = 1.0 / math.sqrt(lax.axis_size("group") * states.shape[0])
    return (
        (grad_total * scale_factor).astype(jnp.bfloat16),
        (target - normed).astype(jnp.bfloat16),
    )


LANES = 128
MIB = 1 << 20
IN_VMEM = pl.BlockSpec(memory_space=pltpu.VMEM)
IN_SMEM = pl.BlockSpec(memory_space=pltpu.SMEM)
ANYWHERE = pl.BlockSpec(memory_space=pl.ANY)
IN_HBM = pl.BlockSpec(memory_space=pltpu.HBM)


def local_call(kernel, outs, args, specs=None, scratch=(), flops=0, moved=0, limit=8, **extra):
    return pl.pallas_call(
        kernel,
        out_shape=[jax.ShapeDtypeStruct(shape, kind) for shape, kind in outs],
        in_specs=specs or [IN_VMEM] * len(args),
        out_specs=[IN_VMEM] * len(outs),
        scratch_shapes=list(scratch),
        compiler_params=pltpu.CompilerParams(vmem_limit_bytes=limit * MIB),
        cost_estimate=pl.CostEstimate(flops=flops, bytes_accessed=moved, transcendentals=0),
        **extra,
    )(*args)


def path(core, side, far):
    return (core ^ side ^ (far > 0)) | (side << 1) | (far << 2)


def split_kernel(x_ref, near_ref, side_ref, core_ref, sems):
    far, _, part = near_ref.shape
    feat = lax.axis_index("dev")
    copies = []
    for c in range(2):
        for n in range(2):
            for m in range(far):
                out = core_ref.at[n, m] if c else (side_ref if n else near_ref).at[m]
                first = pl.multiple_of((feat ^ path(c, n, m)) * part, part)
                copies.append(
                    pltpu.make_async_copy(x_ref.at[:, pl.ds(first, part)], out, sems.at[len(copies)])
                )
    for copy in copies:
        copy.start()
    for copy in copies:
        copy.wait()


def side_kernel(side_ref, core_ref, out_ref):
    out_ref[0] = side_ref[...]
    out_ref[1] = core_ref[1]


def far_kernel(near_ref, core_ref, side_ref, *outs):
    for m, out in enumerate(outs):
        out[0] = near_ref[m]
        out[1] = core_ref[0, m]
        out[2] = side_ref[0, m]
        out[3] = side_ref[1, m]


def fetch(tiles_ref, out_ref, sems, first):
    count = sems.shape[0]
    rows, width = out_ref.shape[0] // count, out_ref.shape[1]
    copies = []
    for i in range(count):
        part = pl.ds(i * rows, rows)
        copies.append(
            pltpu.make_async_copy(
                tiles_ref.at[part, pl.ds(first, width)], out_ref.at[part], sems.at[i]
            )
        )
        copies[-1].start()
    return copies


def first_kernel(place, unit, owner_ref, tiles_ref, pick_ref, out_ref, owner_here, sem, sems):
    order = pltpu.make_async_copy(owner_ref, owner_here, sem)
    order.start()
    copies = fetch(tiles_ref, out_ref, sems, 0)
    feat, group = lax.axis_index("dev"), lax.axis_index("group")
    row = lax.broadcasted_iota(jnp.int32, pick_ref.shape, 0)
    source = lax.broadcasted_iota(jnp.int32, pick_ref.shape, 1)
    wanted = row
    order.wait()
    for p, shift in enumerate(place):
        slot = owner_here[group, feat ^ shift] ^ feat
        wanted = jnp.where(row // unit == p, row + (slot - p) * unit, wanted)
    pick_ref[...] = jnp.where(source == wanted, 1.0, 0.0).astype(jnp.bfloat16)
    for copy in copies:
        copy.wait()


def second_kernel(first, tiles_ref, out_ref, sems):
    for copy in fetch(tiles_ref, out_ref, sems, first):
        copy.wait()


def order_kernel(pick_ref, *refs):
    sources, (first_ref, second_ref) = refs[:-6], refs[-6:-4]
    lhs_ref, leaving_ref, staying_ref, slots = refs[-4:]
    near, unit = sources[0].shape[0], sources[0].shape[1]
    for m, source in enumerate(sources):
        for k in range(near):
            first = path(k & 1, k >> 1, m) * unit
            slots[first : first + unit, :] = source[k].astype(jnp.float32)
    rows = jnp.dot(
        pick_ref[...], slots[...].astype(jnp.bfloat16), preferred_element_type=jnp.float32
    )
    lhs = rows.astype(jnp.bfloat16)
    lhs_ref[...] = lhs
    half, base = staying_ref.shape[0], 0
    for tiles_ref in (first_ref, second_ref):
        width = tiles_ref.shape[1]
        step = min(width, 512)
        for start in range(0, width, step):
            tiles = tiles_ref[:, start : start + step]
            part = jnp.dot(lhs, tiles, preferred_element_type=jnp.float32)
            cols = slice(base + start, base + start + step)
            staying_ref[:, cols] = part[:half]
            leaving_ref[:, cols] = part[half:].astype(jnp.bfloat16)
        base += width


def halve_kernel(kept_ref, arrived_ref, leaving_ref, staying_ref):
    half, width = staying_ref.shape
    cols = slice(0, width)
    staying_ref[...] = kept_ref[:half, cols] + arrived_ref[:half, cols].astype(jnp.float32)
    leaving_ref[...] = (kept_ref[half:, cols] + arrived_ref[half:, cols].astype(jnp.float32)).astype(
        jnp.bfloat16
    )


def unit_lines(kept_ref, arrived_ref, first, lines):
    count = kept_ref.shape[0]
    depth = lines.shape[0] // count
    for t in range(depth):
        cols = slice(first + t * LANES, first + (t + 1) * LANES)
        total = kept_ref[:, cols] + arrived_ref[:, cols].astype(jnp.float32)
        lines[pl.ds(t, count, stride=depth), :] = total


def far_first_kernel(first, kept_ref, arrived_ref, own_ref, *refs):
    leaving, lines = refs[:-1], refs[-1]
    unit_lines(kept_ref, arrived_ref, first, lines)
    size = own_ref.shape[0] // 2
    for n in range(2):
        for m, out in enumerate((own_ref, *leaving)):
            start = (n * (len(leaving) + 1) + m) * size
            out[n * size : (n + 1) * size, :] = lines[start : start + size].astype(out.dtype)


def units_kernel(kept_ref, arrived_ref, own_ref, *refs):
    leaving, lines = refs[:-1], refs[-1]
    unit_lines(kept_ref, arrived_ref, 0, lines)
    size = own_ref.shape[0]
    for m, out in enumerate((own_ref, *leaving)):
        out[...] = lines[m * size : (m + 1) * size].astype(out.dtype)


def far_sum_kernel(*refs):
    (own_ref, *arrived), (leaving_ref, staying_ref) = refs[:-2], refs[-2:]
    size = staying_ref.shape[0]
    total = own_ref[...]
    for other in arrived:
        total = total + other[...].astype(jnp.float32)
    staying_ref[...] = total[:size]
    leaving_ref[...] = total[size:].astype(jnp.bfloat16)


def target_kernel(rows_ref, out_ref):
    count, width = rows_ref.shape
    depth = width // LANES // 2
    for t in range(2 * depth):
        base = t // depth * count * depth + t % depth
        tile = rows_ref[:, t * LANES : (t + 1) * LANES].astype(jnp.float32)
        out_ref[pl.ds(base, count, stride=depth), :] = tile


def slope_kernel(unit, *refs):
    sums, (target_ref, slope_ref, grad_ref) = refs[:-3], refs[-3:]
    size = sums[0].shape[0]
    totals, targets = [], []
    for half, parts in enumerate((sums[:-2], sums[-2:])):
        total = parts[0][...]
        for other in parts[1:]:
            total = total + other[...].astype(jnp.float32)
        totals.append(total.reshape(unit, -1, LANES))
        targets.append(target_ref[half * size : (half + 1) * size].reshape(unit, -1, LANES))

    def row_sum(parts):
        lines = sum(jnp.sum(part, axis=1, keepdims=True) for part in parts)
        return jnp.sum(lines, axis=2, keepdims=True)

    squares = row_sum([total * total for total in totals])
    products = row_sum([total * target for total, target in zip(totals, targets)])
    root_mean = jnp.sqrt(squares / DS + epsilon)
    inner_mean = (squares / (root_mean * root_mean) - products / root_mean) / DS
    for half, (total, target) in enumerate(zip(totals, targets)):
        rows = slice(half * size, (half + 1) * size)
        normed = total / root_mean
        upstream = normed - target
        value = (upstream - normed * inner_mean) / root_mean
        slope_ref[rows, :] = value.reshape(-1, LANES).astype(jnp.bfloat16)
        grad_ref[rows, :] = (target - normed).reshape(-1, LANES)


def rows_kernel(lines_ref, out_ref):
    count, width = out_ref.shape
    depth = width // LANES // 2
    for t in range(2 * depth):
        base = t // depth * count * depth + t % depth
        tile = lines_ref[pl.ds(base, count, stride=depth), :]
        out_ref[:, t * LANES : (t + 1) * LANES] = tile.astype(jnp.bfloat16)


def line_kernel(units, *refs):
    sources, outs, lines = refs[:units], refs[units:-1], refs[-1]
    size = sources[0].shape[0] // 2
    count, width = outs[0].shape
    depth = width // LANES
    for m, source in enumerate(sources):
        for half in range(2):
            rows = slice(m * size, (m + 1) * size)
            lines[half, rows, :] = source[half * size : (half + 1) * size].astype(jnp.float32)
    for half, out in enumerate(outs):
        for t in range(depth):
            tile = lines[half, pl.ds(t, count, stride=depth), :]
            out[:, t * LANES : (t + 1) * LANES] = tile.astype(jnp.bfloat16)


def turn_kernel(own_ref, other_ref, out_ref):
    half = own_ref.shape[0]
    for i, source in enumerate((own_ref, other_ref)):
        out_ref[:, i * half : (i + 1) * half] = source[...].astype(jnp.float32).T.astype(
            jnp.bfloat16
        )


def grad_kernel(scale, step, per, states_ref, *refs):
    slopes, (out_ref, rhs, staged, sems) = refs[:-4], refs[-4:]
    copies, first = [], 0
    for chunk in range(len(slopes) // per):
        pieces = slopes[chunk * per : (chunk + 1) * per]
        count, width = pieces[0].shape
        for start in range(0, width, step):
            j = first // step
            for i, piece in enumerate(pieces):
                rhs[j % 2, i * count : (i + 1) * count, :] = piece[:, start : start + step]
            part = jnp.dot(states_ref[...], rhs[j % 2], preferred_element_type=jnp.float32)
            staged[j] = (part * scale).astype(jnp.bfloat16)
            copies.append(
                pltpu.make_async_copy(staged.at[j], out_ref.at[:, pl.ds(first, step)], sems.at[j])
            )
            copies[-1].start()
            first += step
    for copy in copies:
        copy.wait()


def grad_call(scale, states, slopes, per, shape, step=256):
    block_teacher, rows = states.shape
    count = shape[1] // step
    return pl.pallas_call(
        functools.partial(grad_kernel, scale, step, per),
        out_shape=jax.ShapeDtypeStruct(shape, jnp.bfloat16),
        in_specs=[IN_VMEM] * (len(slopes) + 1),
        out_specs=ANYWHERE,
        scratch_shapes=[
            pltpu.VMEM((2, rows, step), jnp.bfloat16),
            pltpu.VMEM((count, block_teacher, step), jnp.bfloat16),
            pltpu.SemaphoreType.DMA((count,)),
        ],
        compiler_params=pltpu.CompilerParams(vmem_limit_bytes=16 * MIB),
        cost_estimate=pl.CostEstimate(
            flops=2 * rows * block_teacher * shape[1],
            bytes_accessed=2 * block_teacher * shape[1],
            transcendentals=0,
        ),
    )(states, *slopes)


def far_across(values):
    arrived = []
    for m in range(1, len(values)):
        arrived.append(across(values[m], 0, path(0, 0, m)))
    return arrived


def line_shards(teacher, owner, proj_tiles, student_tiles):
    unit, _ = teacher.shape
    block_teacher, block_student = proj_tiles.shape
    near, far = NEAR, FEAT_SPLIT // NEAR
    half = FEAT_SPLIT * unit
    cut = block_student // 2
    depth = cut // LANES
    size = 2 * unit * depth
    bf16, f32 = jnp.bfloat16, jnp.float32

    place = [path(c, n, m) for c in range(2) for n in range(2) for m in range(far)]

    block = (unit, block_teacher)
    own_near, own_side, leaving = local_call(
        split_kernel,
        [((far, *block), bf16), ((far, *block), bf16), ((2, far, *block), bf16)],
        [pltpu.with_memory_space_constraint(teacher, pltpu.HBM)],
        specs=[IN_HBM],
        scratch=[pltpu.SemaphoreType.DMA((FEAT_SPLIT,))],
    )
    core = across(leaving, 0, 1)
    (leaving,) = local_call(side_kernel, [((2, far, *block), bf16)], [own_side, core])
    side = across(leaving, 0, path(0, 1, 0))
    held = local_call(far_kernel, [((near, *block), bf16)] * far, [own_near, core, side])
    held = [held[0]] + far_across(held)

    tiles = pltpu.with_memory_space_constraint(proj_tiles, pltpu.HBM)
    part = (block_teacher, block_student // 2)
    work = dict(flops=block_teacher * half * block_student, moved=block_teacher * block_student)
    pick, first_tiles = local_call(
        functools.partial(first_kernel, place, unit),
        [((half, half), bf16), (part, bf16)],
        [pltpu.with_memory_space_constraint(owner, pltpu.HBM), tiles],
        specs=[IN_HBM] * 2,
        scratch=[
            pltpu.SMEM(owner.shape, owner.dtype),
            pltpu.SemaphoreType.DMA,
            pltpu.SemaphoreType.DMA((8,)),
        ],
        **work,
    )
    (second_tiles,) = local_call(
        functools.partial(second_kernel, part[1]),
        [(part, bf16)],
        [tiles],
        specs=[IN_HBM],
        scratch=[pltpu.SemaphoreType.DMA((8,))],
        **work,
    )
    states, leaving, staying = local_call(
        order_kernel,
        [
            ((half, block_teacher), bf16),
            ((half // 2, block_student), bf16),
            ((half // 2, block_student), f32),
        ],
        [pick, *held, first_tiles, second_tiles],
        scratch=[pltpu.VMEM((half, block_teacher), f32)],
        flops=2 * half * block_teacher * block_student,
    )

    arrived = across(leaving, 0, 1)
    small = size // 2
    kept, swapped = staying, arrived
    leaving, staying = local_call(
        halve_kernel, [((half // 4, cut), bf16), ((half // 4, cut), f32)], [kept, swapped]
    )
    arrived = across(leaving, 0, path(0, 1, 0))
    own, *leaving = local_call(
        functools.partial(far_first_kernel, cut),
        [((size, LANES), f32)] + [((size, LANES), bf16)] * (far - 1),
        [kept, swapped],
        scratch=[pltpu.VMEM((half // 2 * depth, LANES), f32)],
    )
    far_b = far_across([own, *leaving])
    own_a, *leaving = local_call(
        units_kernel,
        [((small, LANES), f32)] + [((small, LANES), bf16)] * (far - 1),
        [staying, arrived],
        scratch=[pltpu.VMEM((half // 4 * depth, LANES), f32)],
    )
    far_a = far_across([own_a, *leaving])
    leaving, own_b = local_call(
        far_sum_kernel, [((small, LANES), bf16), ((small, LANES), f32)], [own, *far_b]
    )
    near_b = across(leaving, 0, path(0, 1, 0))
    (target,) = local_call(target_kernel, [((size, LANES), f32)], [student_tiles])
    slope, grad = local_call(
        functools.partial(slope_kernel, unit),
        [((size, LANES), bf16), ((size, LANES), f32)],
        [own_a, *far_a, own_b, near_b, target],
    )
    (grad,) = local_call(rows_kernel, [((unit, block_student), bf16)], [grad])
    states_too, _ = lax.optimization_barrier((states, slope))
    other_states = across(states_too, 1, 0)

    line = [slope] + far_across([slope] * far)
    lines = local_call(
        functools.partial(line_kernel, far),
        [((far * unit, cut), bf16)] * 2,
        line,
        scratch=[pltpu.VMEM((2, far * small, LANES), f32)],
    )
    scale = 1.0 / math.sqrt(lax.axis_size("group") * half)
    first, second = lines
    first_group, second_near = across(first, 1, 1), across(second, 0, 3)
    second_group, first_near = across(second, 1, 1), across(first, 0, 3)
    first_both, second_both = across(first_group, 0, 3), across(second_near, 1, 1)
    (turned,) = local_call(turn_kernel, [((block_teacher, 2 * half), bf16)], [states, other_states])
    pieces = []
    for own, other in (
        ((first, first_near), (first_group, first_both)),
        ((second, second_near), (second_group, second_both)),
    ):
        pieces += [*own, *[across(piece, 0, 1) for piece in own]]
        pieces += [*[across(piece, 0, 1) for piece in other], *other]
    grad_proj = grad_call(scale, turned, pieces, len(pieces) // 2, (block_teacher, block_student))
    return grad_proj, grad


def shards(*blocks):
    if lax.axis_size("dev") == FEAT_SPLIT:
        return line_shards(*blocks)
    return wide_shards(*blocks)


def solution(mesh):
    placed = (P(("group", "dev"), None), P(), P("dev", None), P(("group", "dev"), None))
    return jax.shard_map(
        shards,
        mesh=mesh,
        in_specs=placed,
        out_specs=(P("dev", None), P(("group", "dev"), None)),
        check_vma=False,
    )
```

```python
import functools
import math

import jax
import jax.numpy as jnp
from jax import lax
from jax.experimental import pallas as pl
from jax.experimental.pallas import tpu as pltpu
from jax.sharding import PartitionSpec as P


DS = 4096
FEAT_SPLIT = 16
NEAR = 4


epsilon = 1e-06


def across(value, group_mask, dev_mask):
    groups, devices = lax.axis_size("group"), lax.axis_size("dev")
    pairs = [
        (g * devices + d, (g ^ group_mask) * devices + (d ^ dev_mask))
        for g in range(groups)
        for d in range(devices)
    ]
    return lax.ppermute(value, ("group", "dev"), pairs)


def gather_wide(block, column_index, spread):
    step = 1
    while step < spread:
        arrived = across(block, 0, step * FEAT_SPLIT)
        my_bit = (column_index & step) > 0
        block = jnp.concatenate(
            [jnp.where(my_bit, arrived, block), jnp.where(my_bit, block, arrived)], axis=0
        )
        step *= 2
    return block


def wide_shards(teacher, owner, proj_tiles, student_tiles):
    row_count, width = teacher.shape
    device_count = lax.axis_size("dev")
    spread = device_count // FEAT_SPLIT
    block_teacher = width // FEAT_SPLIT
    block_student = proj_tiles.shape[1]
    unit = spread * row_count
    far = FEAT_SPLIT // NEAR
    dev_index = lax.axis_index("dev")
    feat_index = dev_index % FEAT_SPLIT
    column_index = dev_index // FEAT_SPLIT
    group_index = lax.axis_index("group")

    full_rows = gather_wide(teacher, column_index, spread)
    pieces = full_rows.reshape(unit, FEAT_SPLIT, block_teacher).transpose(1, 0, 2)
    relative = jnp.arange(FEAT_SPLIT)
    pieces = jnp.take(pieces, feat_index ^ relative, axis=0)
    pieces = pieces.reshape(far, NEAR, unit, block_teacher)
    held = jnp.stack(
        [pieces[0]] + [across(pieces[m], 0, m * NEAR) for m in range(1, far)]
    )
    slots = jnp.stack(
        [held[:, 0]] + [across(held[:, m], 0, m) for m in range(1, NEAR)]
    )
    slots = slots.transpose(1, 0, 2, 3).reshape(device_count, row_count, block_teacher)

    place = jnp.array(
        [c | (n << 1) | (f << 2) for c in range(2) for n in range(NEAR // 2) for f in range(far)]
    )
    owner_row = lax.dynamic_index_in_dim(owner, group_index, 0, keepdims=False)
    student_block = ((feat_index ^ place)[:, None] * spread + jnp.arange(spread)[None]).reshape(-1)
    teacher_block = owner_row[student_block]
    slot = ((teacher_block % FEAT_SPLIT) ^ feat_index) * spread + teacher_block // FEAT_SPLIT
    states = jnp.take(slots, slot, axis=0).reshape(device_count * row_count, block_teacher)
    other_states = across(states, 1, 0)

    partial_value = jnp.dot(states, proj_tiles, preferred_element_type=jnp.float32)
    partial_value = partial_value.reshape(2, -1, block_student)
    for mask in (1, 2):
        arrived = across(partial_value[1].astype(jnp.bfloat16), 0, mask)
        partial_value = (partial_value[0] + arrived.astype(jnp.float32)).reshape(
            2, -1, block_student
        )
    partial_value = partial_value.reshape(far, unit, block_student)
    projected = partial_value[0]
    leaving = partial_value.astype(jnp.bfloat16)
    for m in range(1, far):
        projected = projected + across(leaving[m], 0, m * NEAR).astype(jnp.float32)

    target = student_tiles.astype(jnp.float32)
    row_sums = jnp.stack(
        [jnp.sum(projected * projected, axis=1), jnp.sum(target * projected, axis=1)]
    )
    step = 1
    while step < spread:
        row_sums = row_sums + across(row_sums, 0, step * FEAT_SPLIT)
        step *= 2
    root_mean = jnp.sqrt(row_sums[0] / DS + epsilon)
    normed = projected / root_mean[:, None]
    inner_mean = (row_sums[0] / (root_mean * root_mean) - row_sums[1] / root_mean) / DS
    upstream = normed - target
    row_slope = ((upstream - normed * inner_mean[:, None]) / root_mean[:, None]).astype(
        jnp.bfloat16
    )

    line = jnp.concatenate(
        [row_slope] + [across(row_slope, 0, m * NEAR) for m in range(1, far)], axis=0
    )
    own = [line, across(line, 0, 2)]
    other = [across(line, 1, 0), across(line, 1, 2)]
    own, other = jnp.concatenate(own), jnp.concatenate(other)
    slopes = jnp.concatenate([own, across(own, 0, 1), other, across(other, 0, 1)])
    grad_total = lax.dot_general(
        jnp.concatenate([states, other_states]),
        slopes,
        (((0,), (0,)), ((), ())),
        preferred_element_type=jnp.float32,
    )
    scale_factor = 1.0 / math.sqrt(lax.axis_size("group") * states.shape[0])
    return (
        (grad_total * scale_factor).astype(jnp.bfloat16),
        (target - normed).astype(jnp.bfloat16),
    )


LANES = 128
MIB = 1 << 20
IN_VMEM = pl.BlockSpec(memory_space=pltpu.VMEM)
IN_SMEM = pl.BlockSpec(memory_space=pltpu.SMEM)
ANYWHERE = pl.BlockSpec(memory_space=pl.ANY)
IN_HBM = pl.BlockSpec(memory_space=pltpu.HBM)


def local_call(kernel, outs, args, specs=None, scratch=(), flops=0, moved=0, limit=8, **extra):
    return pl.pallas_call(
        kernel,
        out_shape=[jax.ShapeDtypeStruct(shape, kind) for shape, kind in outs],
        in_specs=specs or [IN_VMEM] * len(args),
        out_specs=[IN_VMEM] * len(outs),
        scratch_shapes=list(scratch),
        compiler_params=pltpu.CompilerParams(vmem_limit_bytes=limit * MIB),
        cost_estimate=pl.CostEstimate(flops=flops, bytes_accessed=moved, transcendentals=0),
        **extra,
    )(*args)


def path(core, side, far):
    return (core ^ side ^ (far > 0)) | (side << 1) | (far << 2)


def split_kernel(x_ref, *refs):
    outs, sems = refs[:-1], refs[-1]
    far, _, part = outs[0].shape
    feat = lax.axis_index("dev")
    copies = []
    for s, out in enumerate(outs):
        for m in range(far):
            first = pl.multiple_of((feat ^ s ^ path(0, 0, m)) * part, part)
            copies.append(
                pltpu.make_async_copy(
                    x_ref.at[:, pl.ds(first, part)], out.at[m], sems.at[len(copies)]
                )
            )
    for copy in copies:
        copy.start()
    for copy in copies:
        copy.wait()


def far_kernel(near, *refs):
    sources, outs, rows = refs[:near], refs[near:-1], refs[-1]
    unit = sources[0].shape[1]
    for m, out in enumerate(outs):
        for s, source in enumerate(sources):
            rows[m, s * unit : (s + 1) * unit, :] = source[m].astype(jnp.float32)
        out[...] = rows[m].astype(jnp.bfloat16)


def fetch(tiles_ref, out_ref, sems, first):
    count = sems.shape[0]
    rows, width = out_ref.shape[0] // count, out_ref.shape[1]
    copies = []
    for i in range(count):
        part = pl.ds(i * rows, rows)
        copies.append(
            pltpu.make_async_copy(
                tiles_ref.at[part, pl.ds(first, width)], out_ref.at[part], sems.at[i]
            )
        )
        copies[-1].start()
    return copies


def first_kernel(place, unit, owner_ref, tiles_ref, pick_ref, out_ref, owner_here, sem, sems):
    order = pltpu.make_async_copy(owner_ref, owner_here, sem)
    order.start()
    copies = fetch(tiles_ref, out_ref, sems, 0)
    feat, group = lax.axis_index("dev"), lax.axis_index("group")
    row = lax.broadcasted_iota(jnp.int32, pick_ref.shape, 0)
    source = lax.broadcasted_iota(jnp.int32, pick_ref.shape, 1)
    wanted = row
    order.wait()
    for p, shift in enumerate(place):
        slot = owner_here[group, feat ^ shift] ^ feat
        slot = slot ^ jnp.where(slot >= NEAR, 1, 0)
        wanted = jnp.where(row // unit == p, row + (slot - p) * unit, wanted)
    pick_ref[...] = jnp.where(source == wanted, 1.0, 0.0).astype(jnp.bfloat16)
    for copy in copies:
        copy.wait()


def second_kernel(first, tiles_ref, out_ref, sems):
    for copy in fetch(tiles_ref, out_ref, sems, first):
        copy.wait()


def product(lhs, tiles_ref, leaving_ref, staying_ref):
    half, width = staying_ref.shape
    step = min(width, 512)
    for start in range(0, width, step):
        cols = slice(start, start + step)
        part = jnp.dot(lhs, tiles_ref[:, cols], preferred_element_type=jnp.float32)
        staying_ref[:, cols] = part[:half]
        leaving_ref[:, cols] = part[half:].astype(jnp.bfloat16)


def order_kernel(pick_ref, *refs):
    sources, (tiles_ref, lhs_ref, leaving_ref, staying_ref, slots) = refs[:-5], refs[-5:]
    count = sources[0].shape[0]
    for m, source in enumerate(sources):
        slots[m * count : (m + 1) * count, :] = source[...]
    lhs = jnp.dot(pick_ref[...], slots[...], preferred_element_type=jnp.float32).astype(jnp.bfloat16)
    lhs_ref[...] = lhs
    product(lhs, tiles_ref, leaving_ref, staying_ref)


def rest_kernel(lhs_ref, tiles_ref, leaving_ref, staying_ref):
    product(lhs_ref[...], tiles_ref, leaving_ref, staying_ref)


def halve_kernel(kept_ref, arrived_ref, leaving_ref, staying_ref):
    half, width = staying_ref.shape
    cols = slice(0, width)
    staying_ref[...] = kept_ref[:half, cols] + arrived_ref[:half, cols].astype(jnp.float32)
    leaving_ref[...] = (kept_ref[half:, cols] + arrived_ref[half:, cols].astype(jnp.float32)).astype(
        jnp.bfloat16
    )


def unit_lines(kept_ref, arrived_ref, lines):
    count = kept_ref.shape[0]
    depth = lines.shape[0] // count
    for t in range(depth):
        cols = slice(t * LANES, (t + 1) * LANES)
        total = kept_ref[:, cols] + arrived_ref[:, cols].astype(jnp.float32)
        lines[pl.ds(t, count, stride=depth), :] = total


def far_first_kernel(kept_ref, arrived_ref, own_ref, *refs):
    leaving, lines = refs[:-1], refs[-1]
    unit_lines(kept_ref, arrived_ref, lines)
    size = own_ref.shape[0] // 2
    for n in range(2):
        for m, out in enumerate((own_ref, *leaving)):
            start = (n * (len(leaving) + 1) + m) * size
            out[n * size : (n + 1) * size, :] = lines[start : start + size].astype(out.dtype)


def units_kernel(kept_ref, arrived_ref, own_ref, *refs):
    leaving, lines = refs[:-1], refs[-1]
    unit_lines(kept_ref, arrived_ref, lines)
    size = own_ref.shape[0]
    for m, out in enumerate((own_ref, *leaving)):
        out[...] = lines[m * size : (m + 1) * size].astype(out.dtype)


def far_sum_kernel(*refs):
    (own_ref, *arrived), (leaving_ref, staying_ref) = refs[:-2], refs[-2:]
    size = staying_ref.shape[0]
    total = own_ref[...]
    for other in arrived:
        total = total + other[...].astype(jnp.float32)
    staying_ref[...] = total[:size]
    leaving_ref[...] = total[size:].astype(jnp.bfloat16)


def target_kernel(rows_ref, out_ref):
    count, width = rows_ref.shape
    depth = width // LANES // 2
    for t in range(2 * depth):
        base = t // depth * count * depth + t % depth
        tile = rows_ref[:, t * LANES : (t + 1) * LANES].astype(jnp.float32)
        out_ref[pl.ds(base, count, stride=depth), :] = tile


def slope_kernel(unit, *refs):
    sums, (target_ref, slope_ref, grad_ref) = refs[:-3], refs[-3:]
    size = sums[0].shape[0]
    totals, targets = [], []
    for half, parts in enumerate((sums[:-2], sums[-2:])):
        total = parts[0][...]
        for other in parts[1:]:
            total = total + other[...].astype(jnp.float32)
        totals.append(total.reshape(unit, -1, LANES))
        targets.append(target_ref[half * size : (half + 1) * size].reshape(unit, -1, LANES))

    def row_sum(parts):
        lines = sum(jnp.sum(part, axis=1, keepdims=True) for part in parts)
        return jnp.sum(lines, axis=2, keepdims=True)

    squares = row_sum([total * total for total in totals])
    products = row_sum([total * target for total, target in zip(totals, targets)])
    root_mean = jnp.sqrt(squares / DS + epsilon)
    inner_mean = (squares / (root_mean * root_mean) - products / root_mean) / DS
    for half, (total, target) in enumerate(zip(totals, targets)):
        rows = slice(half * size, (half + 1) * size)
        normed = total / root_mean
        upstream = normed - target
        value = (upstream - normed * inner_mean) / root_mean
        slope_ref[rows, :] = value.reshape(-1, LANES).astype(jnp.bfloat16)
        grad_ref[rows, :] = (target - normed).reshape(-1, LANES)


def rows_kernel(lines_ref, out_ref):
    count, width = out_ref.shape
    depth = width // LANES // 2
    for t in range(2 * depth):
        base = t // depth * count * depth + t % depth
        tile = lines_ref[pl.ds(base, count, stride=depth), :]
        out_ref[:, t * LANES : (t + 1) * LANES] = tile.astype(jnp.bfloat16)


def line_kernel(units, *refs):
    sources, outs, lines = refs[:units], refs[units:-1], refs[-1]
    size = sources[0].shape[0] // 2
    count, width = outs[0].shape
    depth = width // LANES
    for m, source in enumerate(sources):
        for half in range(2):
            rows = slice(m * size, (m + 1) * size)
            lines[half, rows, :] = source[half * size : (half + 1) * size].astype(jnp.float32)
    for half, out in enumerate(outs):
        for t in range(depth):
            tile = lines[half, pl.ds(t, count, stride=depth), :]
            out[:, t * LANES : (t + 1) * LANES] = tile.astype(jnp.bfloat16)


def turn_kernel(own_ref, other_ref, out_ref):
    half = own_ref.shape[0]
    for i, source in enumerate((own_ref, other_ref)):
        out_ref[:, i * half : (i + 1) * half] = source[...].astype(jnp.float32).T.astype(
            jnp.bfloat16
        )


def grad_kernel(scale, step, per, states_ref, *refs):
    slopes, (out_ref, rhs, staged, sems) = refs[:-4], refs[-4:]
    copies, first = [], 0
    for chunk in range(len(slopes) // per):
        pieces = slopes[chunk * per : (chunk + 1) * per]
        count, width = pieces[0].shape
        for start in range(0, width, step):
            j = first // step
            for i, piece in enumerate(pieces):
                rhs[j % 2, i * count : (i + 1) * count, :] = piece[:, start : start + step]
            part = jnp.dot(states_ref[...], rhs[j % 2], preferred_element_type=jnp.float32)
            staged[j] = (part * scale).astype(jnp.bfloat16)
            copies.append(
                pltpu.make_async_copy(staged.at[j], out_ref.at[:, pl.ds(first, step)], sems.at[j])
            )
            copies[-1].start()
            first += step
    for copy in copies:
        copy.wait()


def grad_call(scale, states, slopes, per, shape, step=512):
    block_teacher, rows = states.shape
    count = shape[1] // step
    return pl.pallas_call(
        functools.partial(grad_kernel, scale, step, per),
        out_shape=jax.ShapeDtypeStruct(shape, jnp.bfloat16),
        in_specs=[IN_VMEM] * (len(slopes) + 1),
        out_specs=ANYWHERE,
        scratch_shapes=[
            pltpu.VMEM((2, rows, step), jnp.bfloat16),
            pltpu.VMEM((count, block_teacher, step), jnp.bfloat16),
            pltpu.SemaphoreType.DMA((count,)),
        ],
        compiler_params=pltpu.CompilerParams(vmem_limit_bytes=16 * MIB),
        cost_estimate=pl.CostEstimate(
            flops=2 * rows * block_teacher * shape[1],
            bytes_accessed=2 * block_teacher * shape[1],
            transcendentals=0,
        ),
    )(states, *slopes)


def far_across(values):
    arrived = []
    for m in range(1, len(values)):
        arrived.append(across(values[m], 0, path(0, 0, m)))
    return arrived


def line_shards(teacher, owner, proj_tiles, student_tiles):
    unit, _ = teacher.shape
    block_teacher, block_student = proj_tiles.shape
    near, far = NEAR, FEAT_SPLIT // NEAR
    half = FEAT_SPLIT * unit
    cut = block_student // 2
    depth = cut // LANES
    size = 2 * unit * depth
    bf16, f32 = jnp.bfloat16, jnp.float32

    place = [path(c, n, m) for c in range(2) for n in range(2) for m in range(far)]

    block = (unit, block_teacher)
    packed = local_call(
        split_kernel,
        [((far, *block), bf16)] * near,
        [pltpu.with_memory_space_constraint(teacher, pltpu.HBM)],
        specs=[IN_HBM],
        scratch=[pltpu.SemaphoreType.DMA((FEAT_SPLIT,))],
    )
    slots = [packed[0]]
    for k in range(1, near):
        slots.append(across(packed[k], 0, k))
    held = local_call(
        functools.partial(far_kernel, near),
        [((near * unit, block_teacher), bf16)] * far,
        slots,
        scratch=[pltpu.VMEM((far, near * unit, block_teacher), f32)],
    )
    held = [held[0]] + far_across(held)

    tiles = pltpu.with_memory_space_constraint(proj_tiles, pltpu.HBM)
    part = (block_teacher, block_student // 2)
    work = dict(flops=block_teacher * half * block_student, moved=block_teacher * block_student)
    pick, first_tiles = local_call(
        functools.partial(first_kernel, place, unit),
        [((half, half), bf16), (part, bf16)],
        [pltpu.with_memory_space_constraint(owner, pltpu.HBM), tiles],
        specs=[IN_HBM] * 2,
        scratch=[
            pltpu.SMEM(owner.shape, owner.dtype),
            pltpu.SemaphoreType.DMA,
            pltpu.SemaphoreType.DMA((8,)),
        ],
        **work,
    )
    (second_tiles,) = local_call(
        functools.partial(second_kernel, part[1]),
        [(part, bf16)],
        [tiles],
        specs=[IN_HBM],
        scratch=[pltpu.SemaphoreType.DMA((8,))],
        **work,
    )
    halves = [((half // 2, cut), bf16), ((half // 2, cut), f32)]
    states, leaving, kept = local_call(
        order_kernel,
        [((half, block_teacher), bf16), *halves],
        [pick, *held, first_tiles],
        scratch=[pltpu.VMEM((half, block_teacher), bf16)],
        **work,
    )
    swapped = across(leaving, 0, 1)
    leaving, kept_b = local_call(rest_kernel, halves, [states, second_tiles], **work)
    swapped_b = across(leaving, 0, 1)
    small = size // 2
    leaving, staying = local_call(
        halve_kernel, [((half // 4, cut), bf16), ((half // 4, cut), f32)], [kept, swapped]
    )
    arrived = across(leaving, 0, path(0, 1, 0))
    own, *leaving = local_call(
        far_first_kernel,
        [((size, LANES), f32)] + [((size, LANES), bf16)] * (far - 1),
        [kept_b, swapped_b],
        scratch=[pltpu.VMEM((half // 2 * depth, LANES), f32)],
    )
    far_b = far_across([own, *leaving])
    own_a, *leaving = local_call(
        units_kernel,
        [((small, LANES), f32)] + [((small, LANES), bf16)] * (far - 1),
        [staying, arrived],
        scratch=[pltpu.VMEM((half // 4 * depth, LANES), f32)],
    )
    far_a = far_across([own_a, *leaving])
    leaving, own_b = local_call(
        far_sum_kernel, [((small, LANES), bf16), ((small, LANES), f32)], [own, *far_b]
    )
    near_b = across(leaving, 0, path(0, 1, 0))
    (target,) = local_call(target_kernel, [((size, LANES), f32)], [student_tiles])
    slope, grad = local_call(
        functools.partial(slope_kernel, unit),
        [((size, LANES), bf16), ((size, LANES), f32)],
        [own_a, *far_a, own_b, near_b, target],
    )
    (grad,) = local_call(rows_kernel, [((unit, block_student), bf16)], [grad])
    states_too, _ = lax.optimization_barrier((states, slope))
    other_states = across(states_too, 1, 0)

    line = [slope] + far_across([slope] * far)
    lines = local_call(
        functools.partial(line_kernel, far),
        [((far * unit, cut), bf16)] * 2,
        line,
        scratch=[pltpu.VMEM((2, far * small, LANES), f32)],
    )
    scale = 1.0 / math.sqrt(lax.axis_size("group") * half)
    first, second = lines
    first_group, second_near = across(first, 1, 1), across(second, 0, 3)
    second_group, first_near = across(second, 1, 1), across(first, 0, 3)
    first_both, second_both = across(first_group, 0, 3), across(second_near, 1, 1)
    (turned,) = local_call(turn_kernel, [((block_teacher, 2 * half), bf16)], [states, other_states])
    pieces = []
    for own, other in (
        ((first, first_near), (first_group, first_both)),
        ((second, second_near), (second_group, second_both)),
    ):
        pieces += [*own, *[across(piece, 0, 1) for piece in own]]
        pieces += [*[across(piece, 0, 1) for piece in other], *other]
    grad_proj = grad_call(scale, turned, pieces, len(pieces) // 2, (block_teacher, block_student))
    return grad_proj, grad


def shards(*blocks):
    if lax.axis_size("dev") == FEAT_SPLIT:
        return line_shards(*blocks)
    return wide_shards(*blocks)


def solution(mesh):
    placed = (P(("group", "dev"), None), P(), P("dev", None), P(("group", "dev"), None))
    return jax.shard_map(
        shards,
        mesh=mesh,
        in_specs=placed,
        out_specs=(P("dev", None), P(("group", "dev"), None)),
        check_vma=False,
    )
```

```python
import functools
import math

import jax
import jax.numpy as jnp
from jax import lax
from jax.experimental import pallas as pl
from jax.experimental.pallas import tpu as pltpu
from jax.sharding import PartitionSpec as P


DS = 4096
FEAT_SPLIT = 16
NEAR = 4


epsilon = 1e-06


def across(value, group_mask, dev_mask):
    groups, devices = lax.axis_size("group"), lax.axis_size("dev")
    pairs = [
        (g * devices + d, (g ^ group_mask) * devices + (d ^ dev_mask))
        for g in range(groups)
        for d in range(devices)
    ]
    return lax.ppermute(value, ("group", "dev"), pairs)


def gather_wide(block, column_index, spread):
    step = 1
    while step < spread:
        arrived = across(block, 0, step * FEAT_SPLIT)
        my_bit = (column_index & step) > 0
        block = jnp.concatenate(
            [jnp.where(my_bit, arrived, block), jnp.where(my_bit, block, arrived)], axis=0
        )
        step *= 2
    return block


def wide_shards(teacher, owner, proj_tiles, student_tiles):
    row_count, width = teacher.shape
    device_count = lax.axis_size("dev")
    spread = device_count // FEAT_SPLIT
    block_teacher = width // FEAT_SPLIT
    block_student = proj_tiles.shape[1]
    unit = spread * row_count
    far = FEAT_SPLIT // NEAR
    dev_index = lax.axis_index("dev")
    feat_index = dev_index % FEAT_SPLIT
    column_index = dev_index // FEAT_SPLIT
    group_index = lax.axis_index("group")

    full_rows = gather_wide(teacher, column_index, spread)
    pieces = full_rows.reshape(unit, FEAT_SPLIT, block_teacher).transpose(1, 0, 2)
    relative = jnp.arange(FEAT_SPLIT)
    pieces = jnp.take(pieces, feat_index ^ relative, axis=0)
    pieces = pieces.reshape(far, NEAR, unit, block_teacher)
    held = jnp.stack(
        [pieces[0]] + [across(pieces[m], 0, m * NEAR) for m in range(1, far)]
    )
    slots = jnp.stack(
        [held[:, 0]] + [across(held[:, m], 0, m) for m in range(1, NEAR)]
    )
    slots = slots.transpose(1, 0, 2, 3).reshape(device_count, row_count, block_teacher)

    place = jnp.array(
        [c | (n << 1) | (f << 2) for c in range(2) for n in range(NEAR // 2) for f in range(far)]
    )
    owner_row = lax.dynamic_index_in_dim(owner, group_index, 0, keepdims=False)
    student_block = ((feat_index ^ place)[:, None] * spread + jnp.arange(spread)[None]).reshape(-1)
    teacher_block = owner_row[student_block]
    slot = ((teacher_block % FEAT_SPLIT) ^ feat_index) * spread + teacher_block // FEAT_SPLIT
    states = jnp.take(slots, slot, axis=0).reshape(device_count * row_count, block_teacher)
    other_states = across(states, 1, 0)

    partial_value = jnp.dot(states, proj_tiles, preferred_element_type=jnp.float32)
    partial_value = partial_value.reshape(2, -1, block_student)
    for mask in (1, 2):
        arrived = across(partial_value[1].astype(jnp.bfloat16), 0, mask)
        partial_value = (partial_value[0] + arrived.astype(jnp.float32)).reshape(
            2, -1, block_student
        )
    partial_value = partial_value.reshape(far, unit, block_student)
    projected = partial_value[0]
    leaving = partial_value.astype(jnp.bfloat16)
    for m in range(1, far):
        projected = projected + across(leaving[m], 0, m * NEAR).astype(jnp.float32)

    target = student_tiles.astype(jnp.float32)
    row_sums = jnp.stack(
        [jnp.sum(projected * projected, axis=1), jnp.sum(target * projected, axis=1)]
    )
    step = 1
    while step < spread:
        row_sums = row_sums + across(row_sums, 0, step * FEAT_SPLIT)
        step *= 2
    root_mean = jnp.sqrt(row_sums[0] / DS + epsilon)
    normed = projected / root_mean[:, None]
    inner_mean = (row_sums[0] / (root_mean * root_mean) - row_sums[1] / root_mean) / DS
    upstream = normed - target
    row_slope = ((upstream - normed * inner_mean[:, None]) / root_mean[:, None]).astype(
        jnp.bfloat16
    )

    line = jnp.concatenate(
        [row_slope] + [across(row_slope, 0, m * NEAR) for m in range(1, far)], axis=0
    )
    own = [line, across(line, 0, 2)]
    other = [across(line, 1, 0), across(line, 1, 2)]
    own, other = jnp.concatenate(own), jnp.concatenate(other)
    slopes = jnp.concatenate([own, across(own, 0, 1), other, across(other, 0, 1)])
    grad_total = lax.dot_general(
        jnp.concatenate([states, other_states]),
        slopes,
        (((0,), (0,)), ((), ())),
        preferred_element_type=jnp.float32,
    )
    scale_factor = 1.0 / math.sqrt(lax.axis_size("group") * states.shape[0])
    return (
        (grad_total * scale_factor).astype(jnp.bfloat16),
        (target - normed).astype(jnp.bfloat16),
    )


LANES = 128
MIB = 1 << 20
IN_VMEM = pl.BlockSpec(memory_space=pltpu.VMEM)
IN_SMEM = pl.BlockSpec(memory_space=pltpu.SMEM)
ANYWHERE = pl.BlockSpec(memory_space=pl.ANY)
IN_HBM = pl.BlockSpec(memory_space=pltpu.HBM)


def local_call(kernel, outs, args, specs=None, scratch=(), flops=0, moved=0, limit=8, **extra):
    return pl.pallas_call(
        kernel,
        out_shape=[jax.ShapeDtypeStruct(shape, kind) for shape, kind in outs],
        in_specs=specs or [IN_VMEM] * len(args),
        out_specs=[IN_VMEM] * len(outs),
        scratch_shapes=list(scratch),
        compiler_params=pltpu.CompilerParams(vmem_limit_bytes=limit * MIB),
        cost_estimate=pl.CostEstimate(flops=flops, bytes_accessed=moved, transcendentals=0),
        **extra,
    )(*args)


def path(core, side, far):
    return (core ^ side ^ (far > 0)) | (side << 1) | (far << 2)


def split_kernel(x_ref, *refs):
    outs, (x, rows, sems) = refs[:-3], refs[-3:]
    unit, part = x.shape[0], outs[0].shape[1]
    feat = lax.axis_index("dev")
    copies = []
    width = x.shape[1] // sems.shape[0]
    for i in range(sems.shape[0]):
        cols = pl.ds(i * width, width)
        copies.append(pltpu.make_async_copy(x_ref.at[:, cols], x.at[:, cols], sems.at[i]))
        copies[-1].start()
    for copy in copies:
        copy.wait()
    for s, out in enumerate(outs):
        for m in range(out.shape[0] // unit):
            first = pl.multiple_of((feat ^ s ^ path(0, 0, m)) * part, part)
            rows[s, m * unit : (m + 1) * unit, :] = x[:, pl.ds(first, part)].astype(jnp.float32)
        out[...] = rows[s].astype(jnp.bfloat16)


def far_kernel(near, *refs):
    sources, outs, (taken, rows) = refs[:near], refs[near:-2], refs[-2:]
    unit = sources[0].shape[0] // len(outs)
    for s, source in enumerate(sources):
        taken[s] = source[...].astype(jnp.float32)
        for m in range(len(outs)):
            rows[m, s * unit : (s + 1) * unit, :] = taken[s, m * unit : (m + 1) * unit, :]
    for m, out in enumerate(outs):
        out[...] = rows[m].astype(jnp.bfloat16)


def fetch(tiles_ref, out_ref, sems, first):
    count = sems.shape[0]
    rows, width = out_ref.shape[0] // count, out_ref.shape[1]
    copies = []
    for i in range(count):
        part = pl.ds(i * rows, rows)
        copies.append(
            pltpu.make_async_copy(
                tiles_ref.at[part, pl.ds(first, width)], out_ref.at[part], sems.at[i]
            )
        )
        copies[-1].start()
    return copies


def first_kernel(place, unit, owner_ref, tiles_ref, pick_ref, out_ref, owner_here, sem, sems):
    order = pltpu.make_async_copy(owner_ref, owner_here, sem)
    order.start()
    copies = fetch(tiles_ref, out_ref, sems, 0)
    feat, group = lax.axis_index("dev"), lax.axis_index("group")
    row = lax.broadcasted_iota(jnp.int32, pick_ref.shape, 0)
    source = lax.broadcasted_iota(jnp.int32, pick_ref.shape, 1)
    wanted = row
    order.wait()
    for p, shift in enumerate(place):
        slot = owner_here[group, feat ^ shift] ^ feat
        slot = slot ^ jnp.where(slot >= NEAR, 1, 0)
        wanted = jnp.where(row // unit == p, row + (slot - p) * unit, wanted)
    pick_ref[...] = jnp.where(source == wanted, 1.0, 0.0).astype(jnp.bfloat16)
    for copy in copies:
        copy.wait()


def second_kernel(first, tiles_ref, out_ref, sems):
    for copy in fetch(tiles_ref, out_ref, sems, first):
        copy.wait()


def product(lhs, tiles_ref, leaving_ref, staying_ref):
    half, width = staying_ref.shape
    step = min(width, 512)
    for start in range(0, width, step):
        cols = slice(start, start + step)
        part = jnp.dot(lhs, tiles_ref[:, cols], preferred_element_type=jnp.float32)
        staying_ref[:, cols] = part[:half]
        leaving_ref[:, cols] = part[half:].astype(jnp.bfloat16)


def order_kernel(pick_ref, *refs):
    sources, (tiles_ref, lhs_ref, leaving_ref, staying_ref, slots) = refs[:-5], refs[-5:]
    count = sources[0].shape[0]
    for m, source in enumerate(sources):
        slots[m * count : (m + 1) * count, :] = source[...]
    lhs = jnp.dot(pick_ref[...], slots[...], preferred_element_type=jnp.float32).astype(jnp.bfloat16)
    lhs_ref[...] = lhs
    product(lhs, tiles_ref, leaving_ref, staying_ref)


def rest_kernel(lhs_ref, tiles_ref, leaving_ref, staying_ref):
    product(lhs_ref[...], tiles_ref, leaving_ref, staying_ref)


def halve_kernel(kept_ref, arrived_ref, leaving_ref, staying_ref):
    half, width = staying_ref.shape
    cols = slice(0, width)
    staying_ref[...] = kept_ref[:half, cols] + arrived_ref[:half, cols].astype(jnp.float32)
    leaving_ref[...] = (kept_ref[half:, cols] + arrived_ref[half:, cols].astype(jnp.float32)).astype(
        jnp.bfloat16
    )


def unit_lines(kept_ref, arrived_ref, lines):
    count = kept_ref.shape[0]
    depth = lines.shape[0] // count
    for t in range(depth):
        cols = slice(t * LANES, (t + 1) * LANES)
        total = kept_ref[:, cols] + arrived_ref[:, cols].astype(jnp.float32)
        lines[pl.ds(t, count, stride=depth), :] = total


def far_first_kernel(kept_ref, arrived_ref, own_ref, *refs):
    leaving, lines = refs[:-1], refs[-1]
    unit_lines(kept_ref, arrived_ref, lines)
    size = own_ref.shape[0] // 2
    for n in range(2):
        for m, out in enumerate((own_ref, *leaving)):
            start = (n * (len(leaving) + 1) + m) * size
            out[n * size : (n + 1) * size, :] = lines[start : start + size].astype(out.dtype)


def units_kernel(kept_ref, arrived_ref, own_ref, *refs):
    leaving, lines = refs[:-1], refs[-1]
    unit_lines(kept_ref, arrived_ref, lines)
    size = own_ref.shape[0]
    for m, out in enumerate((own_ref, *leaving)):
        out[...] = lines[m * size : (m + 1) * size].astype(out.dtype)


def far_sum_kernel(*refs):
    (own_ref, *arrived), (leaving_ref, staying_ref) = refs[:-2], refs[-2:]
    size = staying_ref.shape[0]
    total = own_ref[...]
    for other in arrived:
        total = total + other[...].astype(jnp.float32)
    staying_ref[...] = total[:size]
    leaving_ref[...] = total[size:].astype(jnp.bfloat16)


def target_kernel(rows_ref, out_ref):
    count, width = rows_ref.shape
    depth = width // LANES // 2
    for t in range(2 * depth):
        base = t // depth * count * depth + t % depth
        tile = rows_ref[:, t * LANES : (t + 1) * LANES].astype(jnp.float32)
        out_ref[pl.ds(base, count, stride=depth), :] = tile


def slope_kernel(unit, *refs):
    sums, (target_ref, slope_ref, grad_ref) = refs[:-3], refs[-3:]
    size = sums[0].shape[0]
    totals, targets = [], []
    for half, parts in enumerate((sums[:-2], sums[-2:])):
        total = parts[0][...]
        for other in parts[1:]:
            total = total + other[...].astype(jnp.float32)
        totals.append(total.reshape(unit, -1, LANES))
        targets.append(target_ref[half * size : (half + 1) * size].reshape(unit, -1, LANES))

    def row_sum(parts):
        lines = sum(jnp.sum(part, axis=1, keepdims=True) for part in parts)
        return jnp.sum(lines, axis=2, keepdims=True)

    squares = row_sum([total * total for total in totals])
    products = row_sum([total * target for total, target in zip(totals, targets)])
    root_mean = jnp.sqrt(squares / DS + epsilon)
    inner_mean = (squares / (root_mean * root_mean) - products / root_mean) / DS
    for half, (total, target) in enumerate(zip(totals, targets)):
        rows = slice(half * size, (half + 1) * size)
        normed = total / root_mean
        upstream = normed - target
        value = (upstream - normed * inner_mean) / root_mean
        slope_ref[rows, :] = value.reshape(-1, LANES).astype(jnp.bfloat16)
        grad_ref[rows, :] = (target - normed).reshape(-1, LANES)


def rows_kernel(lines_ref, out_ref):
    count, width = out_ref.shape
    depth = width // LANES // 2
    for t in range(2 * depth):
        base = t // depth * count * depth + t % depth
        tile = lines_ref[pl.ds(base, count, stride=depth), :]
        out_ref[:, t * LANES : (t + 1) * LANES] = tile.astype(jnp.bfloat16)


def line_kernel(units, *refs):
    sources, outs, lines = refs[:units], refs[units:-1], refs[-1]
    size = sources[0].shape[0] // 2
    count, width = outs[0].shape
    depth = width // LANES
    for m, source in enumerate(sources):
        for half in range(2):
            rows = slice(m * size, (m + 1) * size)
            lines[half, rows, :] = source[half * size : (half + 1) * size].astype(jnp.float32)
    for half, out in enumerate(outs):
        for t in range(depth):
            tile = lines[half, pl.ds(t, count, stride=depth), :]
            out[:, t * LANES : (t + 1) * LANES] = tile.astype(jnp.bfloat16)


def turn_kernel(own_ref, other_ref, out_ref):
    half = own_ref.shape[0]
    for i, source in enumerate((own_ref, other_ref)):
        out_ref[:, i * half : (i + 1) * half] = source[...].astype(jnp.float32).T.astype(
            jnp.bfloat16
        )


def grad_kernel(scale, step, per, states_ref, *refs):
    slopes, (out_ref, rhs, staged, sems) = refs[:-4], refs[-4:]
    copies, first = [], 0
    for chunk in range(len(slopes) // per):
        pieces = slopes[chunk * per : (chunk + 1) * per]
        count, width = pieces[0].shape
        for start in range(0, width, step):
            j = first // step
            for i, piece in enumerate(pieces):
                rhs[j % 2, i * count : (i + 1) * count, :] = piece[:, start : start + step]
            part = jnp.dot(states_ref[...], rhs[j % 2], preferred_element_type=jnp.float32)
            staged[j] = (part * scale).astype(jnp.bfloat16)
            copies.append(
                pltpu.make_async_copy(staged.at[j], out_ref.at[:, pl.ds(first, step)], sems.at[j])
            )
            copies[-1].start()
            first += step
    for copy in copies:
        copy.wait()


def grad_call(scale, states, slopes, per, shape, step=512):
    block_teacher, rows = states.shape
    count = shape[1] // step
    return pl.pallas_call(
        functools.partial(grad_kernel, scale, step, per),
        out_shape=jax.ShapeDtypeStruct(shape, jnp.bfloat16),
        in_specs=[IN_VMEM] * (len(slopes) + 1),
        out_specs=ANYWHERE,
        scratch_shapes=[
            pltpu.VMEM((2, rows, step), jnp.bfloat16),
            pltpu.VMEM((count, block_teacher, step), jnp.bfloat16),
            pltpu.SemaphoreType.DMA((count,)),
        ],
        compiler_params=pltpu.CompilerParams(vmem_limit_bytes=16 * MIB),
        cost_estimate=pl.CostEstimate(
            flops=2 * rows * block_teacher * shape[1],
            bytes_accessed=2 * block_teacher * shape[1],
            transcendentals=0,
        ),
    )(states, *slopes)


def far_across(values):
    arrived = []
    for m in range(1, len(values)):
        arrived.append(across(values[m], 0, path(0, 0, m)))
    return arrived


def line_shards(teacher, owner, proj_tiles, student_tiles):
    unit, _ = teacher.shape
    block_teacher, block_student = proj_tiles.shape
    near, far = NEAR, FEAT_SPLIT // NEAR
    half = FEAT_SPLIT * unit
    cut = block_student // 2
    depth = cut // LANES
    size = 2 * unit * depth
    bf16, f32 = jnp.bfloat16, jnp.float32

    place = [path(c, n, m) for c in range(2) for n in range(2) for m in range(far)]

    rows = (near * unit, block_teacher)
    packed = local_call(
        split_kernel,
        [((far * unit, block_teacher), bf16)] * near,
        [pltpu.with_memory_space_constraint(teacher, pltpu.HBM)],
        specs=[IN_HBM],
        scratch=[
            pltpu.VMEM(teacher.shape, bf16),
            pltpu.VMEM((near, far * unit, block_teacher), f32),
            pltpu.SemaphoreType.DMA((4,)),
        ],
    )
    slots = [packed[0]]
    for k in range(1, near):
        slots.append(across(packed[k], 0, k))
    held = local_call(
        functools.partial(far_kernel, near),
        [(rows, bf16)] * far,
        slots,
        scratch=[
            pltpu.VMEM((near, far * unit, block_teacher), f32),
            pltpu.VMEM((far, *rows), f32),
        ],
    )
    held = [held[0]] + far_across(held)

    tiles = pltpu.with_memory_space_constraint(proj_tiles, pltpu.HBM)
    part = (block_teacher, block_student // 2)
    work = dict(flops=block_teacher * half * block_student, moved=block_teacher * block_student)
    pick, first_tiles = local_call(
        functools.partial(first_kernel, place, unit),
        [((half, half), bf16), (part, bf16)],
        [pltpu.with_memory_space_constraint(owner, pltpu.HBM), tiles],
        specs=[IN_HBM] * 2,
        scratch=[
            pltpu.SMEM(owner.shape, owner.dtype),
            pltpu.SemaphoreType.DMA,
            pltpu.SemaphoreType.DMA((8,)),
        ],
        **work,
    )
    (second_tiles,) = local_call(
        functools.partial(second_kernel, part[1]),
        [(part, bf16)],
        [tiles],
        specs=[IN_HBM],
        scratch=[pltpu.SemaphoreType.DMA((8,))],
        **work,
    )
    halves = [((half // 2, cut), bf16), ((half // 2, cut), f32)]
    states, leaving, kept = local_call(
        order_kernel,
        [((half, block_teacher), bf16), *halves],
        [pick, *held, first_tiles],
        scratch=[pltpu.VMEM((half, block_teacher), bf16)],
        **work,
    )
    swapped = across(leaving, 0, 1)
    leaving, kept_b = local_call(rest_kernel, halves, [states, second_tiles], **work)
    swapped_b = across(leaving, 0, 1)
    small = size // 2
    leaving, staying = local_call(
        halve_kernel, [((half // 4, cut), bf16), ((half // 4, cut), f32)], [kept, swapped]
    )
    arrived = across(leaving, 0, path(0, 1, 0))
    own, *leaving = local_call(
        far_first_kernel,
        [((size, LANES), f32)] + [((size, LANES), bf16)] * (far - 1),
        [kept_b, swapped_b],
        scratch=[pltpu.VMEM((half // 2 * depth, LANES), f32)],
    )
    far_b = far_across([own, *leaving])
    own_a, *leaving = local_call(
        units_kernel,
        [((small, LANES), f32)] + [((small, LANES), bf16)] * (far - 1),
        [staying, arrived],
        scratch=[pltpu.VMEM((half // 4 * depth, LANES), f32)],
    )
    far_a = far_across([own_a, *leaving])
    leaving, own_b = local_call(
        far_sum_kernel, [((small, LANES), bf16), ((small, LANES), f32)], [own, *far_b]
    )
    near_b = across(leaving, 0, path(0, 1, 0))
    (target,) = local_call(target_kernel, [((size, LANES), f32)], [student_tiles])
    other_states = across(states, 1, 0)
    slope, grad = local_call(
        functools.partial(slope_kernel, unit),
        [((size, LANES), bf16), ((size, LANES), f32)],
        [own_a, *far_a, own_b, near_b, target],
    )
    (grad,) = local_call(rows_kernel, [((unit, block_student), bf16)], [grad])

    line = [slope] + far_across([slope] * far)
    lines = local_call(
        functools.partial(line_kernel, far),
        [((far * unit, cut), bf16)] * 2,
        line,
        scratch=[pltpu.VMEM((2, far * small, LANES), f32)],
    )
    scale = 1.0 / math.sqrt(lax.axis_size("group") * half)
    first, second = lines
    first_group, second_near = across(first, 1, 1), across(second, 0, 3)
    second_group, first_near = across(second, 1, 1), across(first, 0, 3)
    first_both, second_both = across(first_group, 0, 3), across(second_near, 1, 1)
    (turned,) = local_call(turn_kernel, [((block_teacher, 2 * half), bf16)], [states, other_states])
    pieces = []
    for own, other in (
        ((first, first_near), (first_group, first_both)),
        ((second, second_near), (second_group, second_both)),
    ):
        pieces += [*own, *[across(piece, 0, 1) for piece in own]]
        pieces += [*[across(piece, 0, 1) for piece in other], *other]
    grad_proj = grad_call(scale, turned, pieces, len(pieces) // 2, (block_teacher, block_student))
    return grad_proj, grad


def shards(*blocks):
    if lax.axis_size("dev") == FEAT_SPLIT:
        return line_shards(*blocks)
    return wide_shards(*blocks)


def solution(mesh):
    placed = (P(("group", "dev"), None), P(), P("dev", None), P(("group", "dev"), None))
    return jax.shard_map(
        shards,
        mesh=mesh,
        in_specs=placed,
        out_specs=(P("dev", None), P(("group", "dev"), None)),
        check_vma=False,
    )
```

```python
import functools
import math

import jax
import jax.numpy as jnp
from jax import lax
from jax.experimental import pallas as pl
from jax.experimental.pallas import tpu as pltpu
from jax.sharding import PartitionSpec as P


DS = 4096
FEAT_SPLIT = 16
NEAR = 4


epsilon = 1e-06


def across(value, group_mask, dev_mask):
    groups, devices = lax.axis_size("group"), lax.axis_size("dev")
    pairs = [
        (g * devices + d, (g ^ group_mask) * devices + (d ^ dev_mask))
        for g in range(groups)
        for d in range(devices)
    ]
    return lax.ppermute(value, ("group", "dev"), pairs)


def gather_wide(block, column_index, spread):
    step = 1
    while step < spread:
        arrived = across(block, 0, step * FEAT_SPLIT)
        my_bit = (column_index & step) > 0
        block = jnp.concatenate(
            [jnp.where(my_bit, arrived, block), jnp.where(my_bit, block, arrived)], axis=0
        )
        step *= 2
    return block


def wide_shards(teacher, owner, proj_tiles, student_tiles):
    row_count, width = teacher.shape
    device_count = lax.axis_size("dev")
    spread = device_count // FEAT_SPLIT
    block_teacher = width // FEAT_SPLIT
    block_student = proj_tiles.shape[1]
    unit = spread * row_count
    far = FEAT_SPLIT // NEAR
    dev_index = lax.axis_index("dev")
    feat_index = dev_index % FEAT_SPLIT
    column_index = dev_index // FEAT_SPLIT
    group_index = lax.axis_index("group")

    full_rows = gather_wide(teacher, column_index, spread)
    pieces = full_rows.reshape(unit, FEAT_SPLIT, block_teacher).transpose(1, 0, 2)
    relative = jnp.arange(FEAT_SPLIT)
    pieces = jnp.take(pieces, feat_index ^ relative, axis=0)
    pieces = pieces.reshape(far, NEAR, unit, block_teacher)
    held = jnp.stack(
        [pieces[0]] + [across(pieces[m], 0, m * NEAR) for m in range(1, far)]
    )
    slots = jnp.stack(
        [held[:, 0]] + [across(held[:, m], 0, m) for m in range(1, NEAR)]
    )
    slots = slots.transpose(1, 0, 2, 3).reshape(device_count, row_count, block_teacher)

    place = jnp.array(
        [c | (n << 1) | (f << 2) for c in range(2) for n in range(NEAR // 2) for f in range(far)]
    )
    owner_row = lax.dynamic_index_in_dim(owner, group_index, 0, keepdims=False)
    student_block = ((feat_index ^ place)[:, None] * spread + jnp.arange(spread)[None]).reshape(-1)
    teacher_block = owner_row[student_block]
    slot = ((teacher_block % FEAT_SPLIT) ^ feat_index) * spread + teacher_block // FEAT_SPLIT
    states = jnp.take(slots, slot, axis=0).reshape(device_count * row_count, block_teacher)
    other_states = across(states, 1, 0)

    partial_value = jnp.dot(states, proj_tiles, preferred_element_type=jnp.float32)
    partial_value = partial_value.reshape(2, -1, block_student)
    for mask in (1, 2):
        arrived = across(partial_value[1].astype(jnp.bfloat16), 0, mask)
        partial_value = (partial_value[0] + arrived.astype(jnp.float32)).reshape(
            2, -1, block_student
        )
    partial_value = partial_value.reshape(far, unit, block_student)
    projected = partial_value[0]
    leaving = partial_value.astype(jnp.bfloat16)
    for m in range(1, far):
        projected = projected + across(leaving[m], 0, m * NEAR).astype(jnp.float32)

    target = student_tiles.astype(jnp.float32)
    row_sums = jnp.stack(
        [jnp.sum(projected * projected, axis=1), jnp.sum(target * projected, axis=1)]
    )
    step = 1
    while step < spread:
        row_sums = row_sums + across(row_sums, 0, step * FEAT_SPLIT)
        step *= 2
    root_mean = jnp.sqrt(row_sums[0] / DS + epsilon)
    normed = projected / root_mean[:, None]
    inner_mean = (row_sums[0] / (root_mean * root_mean) - row_sums[1] / root_mean) / DS
    upstream = normed - target
    row_slope = ((upstream - normed * inner_mean[:, None]) / root_mean[:, None]).astype(
        jnp.bfloat16
    )

    line = jnp.concatenate(
        [row_slope] + [across(row_slope, 0, m * NEAR) for m in range(1, far)], axis=0
    )
    own = [line, across(line, 0, 2)]
    other = [across(line, 1, 0), across(line, 1, 2)]
    own, other = jnp.concatenate(own), jnp.concatenate(other)
    slopes = jnp.concatenate([own, across(own, 0, 1), other, across(other, 0, 1)])
    grad_total = lax.dot_general(
        jnp.concatenate([states, other_states]),
        slopes,
        (((0,), (0,)), ((), ())),
        preferred_element_type=jnp.float32,
    )
    scale_factor = 1.0 / math.sqrt(lax.axis_size("group") * states.shape[0])
    return (
        (grad_total * scale_factor).astype(jnp.bfloat16),
        (target - normed).astype(jnp.bfloat16),
    )


LANES = 128
MIB = 1 << 20
IN_VMEM = pl.BlockSpec(memory_space=pltpu.VMEM)
IN_SMEM = pl.BlockSpec(memory_space=pltpu.SMEM)
ANYWHERE = pl.BlockSpec(memory_space=pl.ANY)
IN_HBM = pl.BlockSpec(memory_space=pltpu.HBM)


def local_call(kernel, outs, args, specs=None, scratch=(), flops=0, moved=0, limit=8, **extra):
    return pl.pallas_call(
        kernel,
        out_shape=[jax.ShapeDtypeStruct(shape, kind) for shape, kind in outs],
        in_specs=specs or [IN_VMEM] * len(args),
        out_specs=[IN_VMEM] * len(outs),
        scratch_shapes=list(scratch),
        compiler_params=pltpu.CompilerParams(vmem_limit_bytes=limit * MIB),
        cost_estimate=pl.CostEstimate(flops=flops, bytes_accessed=moved, transcendentals=0),
        **extra,
    )(*args)


def path(core, side, far):
    return (core ^ side ^ (far > 0)) | (side << 1) | (far << 2)


def split_kernel(x_ref, *refs):
    outs, (x, rows, sems) = refs[:-3], refs[-3:]
    unit, part = x.shape[0], outs[0].shape[1]
    feat = lax.axis_index("dev")
    copies = []
    width = x.shape[1] // sems.shape[0]
    for i in range(sems.shape[0]):
        cols = pl.ds(i * width, width)
        copies.append(pltpu.make_async_copy(x_ref.at[:, cols], x.at[:, cols], sems.at[i]))
        copies[-1].start()
    for copy in copies:
        copy.wait()
    for s, out in enumerate(outs):
        for m in range(out.shape[0] // unit):
            first = pl.multiple_of((feat ^ s ^ path(0, 0, m)) * part, part)
            rows[s, m * unit : (m + 1) * unit, :] = x[:, pl.ds(first, part)].astype(jnp.float32)
        out[...] = rows[s].astype(jnp.bfloat16)


def far_kernel(near, *refs):
    sources, outs, (taken, rows) = refs[:near], refs[near:-2], refs[-2:]
    unit = sources[0].shape[0] // len(outs)
    for s, source in enumerate(sources):
        taken[s] = source[...].astype(jnp.float32)
        for m in range(len(outs)):
            rows[m, s * unit : (s + 1) * unit, :] = taken[s, m * unit : (m + 1) * unit, :]
    for m, out in enumerate(outs):
        out[...] = rows[m].astype(jnp.bfloat16)


def fetch(tiles_ref, out_ref, sems, first):
    count = sems.shape[0]
    rows, width = out_ref.shape[0] // count, out_ref.shape[1]
    copies = []
    for i in range(count):
        part = pl.ds(i * rows, rows)
        copies.append(
            pltpu.make_async_copy(
                tiles_ref.at[part, pl.ds(first, width)], out_ref.at[part], sems.at[i]
            )
        )
        copies[-1].start()
    return copies


def first_kernel(place, unit, owner_ref, tiles_ref, pick_ref, out_ref, owner_here, sem, sems):
    order = pltpu.make_async_copy(owner_ref, owner_here, sem)
    order.start()
    copies = fetch(tiles_ref, out_ref, sems, 0)
    feat, group = lax.axis_index("dev"), lax.axis_index("group")
    row = lax.broadcasted_iota(jnp.int32, pick_ref.shape, 0)
    source = lax.broadcasted_iota(jnp.int32, pick_ref.shape, 1)
    wanted = row
    order.wait()
    for p, shift in enumerate(place):
        slot = owner_here[group, feat ^ shift] ^ feat
        slot = slot ^ jnp.where(slot >= NEAR, 1, 0)
        wanted = jnp.where(row // unit == p, row + (slot - p) * unit, wanted)
    pick_ref[...] = jnp.where(source == wanted, 1.0, 0.0).astype(jnp.bfloat16)
    for copy in copies:
        copy.wait()


def second_kernel(first, tiles_ref, out_ref, sems):
    for copy in fetch(tiles_ref, out_ref, sems, first):
        copy.wait()


def product(lhs, tiles_ref, leaving_ref, staying_ref):
    half, width = staying_ref.shape
    step = min(width, 512)
    for start in range(0, width, step):
        cols = slice(start, start + step)
        part = jnp.dot(lhs, tiles_ref[:, cols], preferred_element_type=jnp.float32)
        staying_ref[:, cols] = part[:half]
        leaving_ref[:, cols] = part[half:].astype(jnp.bfloat16)


def order_kernel(pick_ref, *refs):
    sources, (tiles_ref, lhs_ref, leaving_ref, staying_ref, slots) = refs[:-5], refs[-5:]
    count = sources[0].shape[0]
    for m, source in enumerate(sources):
        slots[m * count : (m + 1) * count, :] = source[...]
    lhs = jnp.dot(pick_ref[...], slots[...], preferred_element_type=jnp.float32).astype(jnp.bfloat16)
    lhs_ref[...] = lhs
    product(lhs, tiles_ref, leaving_ref, staying_ref)


def rest_kernel(lhs_ref, tiles_ref, leaving_ref, staying_ref):
    product(lhs_ref[...], tiles_ref, leaving_ref, staying_ref)


def halve_kernel(kept_ref, arrived_ref, leaving_ref, staying_ref):
    half, width = staying_ref.shape
    cols = slice(0, width)
    staying_ref[...] = kept_ref[:half, cols] + arrived_ref[:half, cols].astype(jnp.float32)
    leaving_ref[...] = (kept_ref[half:, cols] + arrived_ref[half:, cols].astype(jnp.float32)).astype(
        jnp.bfloat16
    )


def unit_lines(kept_ref, arrived_ref, lines):
    count = kept_ref.shape[0]
    depth = lines.shape[0] // count
    for t in range(depth):
        cols = slice(t * LANES, (t + 1) * LANES)
        total = kept_ref[:, cols] + arrived_ref[:, cols].astype(jnp.float32)
        lines[pl.ds(t, count, stride=depth), :] = total


def far_first_kernel(kept_ref, arrived_ref, own_ref, *refs):
    leaving, lines = refs[:-1], refs[-1]
    unit_lines(kept_ref, arrived_ref, lines)
    size = own_ref.shape[0] // 2
    for n in range(2):
        for m, out in enumerate((own_ref, *leaving)):
            start = (n * (len(leaving) + 1) + m) * size
            out[n * size : (n + 1) * size, :] = lines[start : start + size].astype(out.dtype)


def units_kernel(kept_ref, arrived_ref, own_ref, *refs):
    leaving, lines = refs[:-1], refs[-1]
    unit_lines(kept_ref, arrived_ref, lines)
    size = own_ref.shape[0]
    for m, out in enumerate((own_ref, *leaving)):
        out[...] = lines[m * size : (m + 1) * size].astype(out.dtype)


def far_sum_kernel(*refs):
    (own_ref, *arrived), (leaving_ref, staying_ref) = refs[:-2], refs[-2:]
    size = staying_ref.shape[0]
    total = own_ref[...]
    for other in arrived:
        total = total + other[...].astype(jnp.float32)
    staying_ref[...] = total[:size]
    leaving_ref[...] = total[size:].astype(jnp.bfloat16)


def target_kernel(rows_ref, out_ref):
    count, width = rows_ref.shape
    depth = width // LANES // 2
    for t in range(2 * depth):
        base = t // depth * count * depth + t % depth
        tile = rows_ref[:, t * LANES : (t + 1) * LANES].astype(jnp.float32)
        out_ref[pl.ds(base, count, stride=depth), :] = tile


def slope_kernel(unit, *refs):
    sums, (target_ref, slope_ref, grad_ref) = refs[:-3], refs[-3:]
    size = sums[0].shape[0]
    totals, targets = [], []
    for half, parts in enumerate((sums[:-2], sums[-2:])):
        total = parts[0][...]
        for other in parts[1:]:
            total = total + other[...].astype(jnp.float32)
        totals.append(total.reshape(unit, -1, LANES))
        targets.append(target_ref[half * size : (half + 1) * size].reshape(unit, -1, LANES))

    def row_sum(parts):
        lines = sum(jnp.sum(part, axis=1, keepdims=True) for part in parts)
        return jnp.sum(lines, axis=2, keepdims=True)

    squares = row_sum([total * total for total in totals])
    products = row_sum([total * target for total, target in zip(totals, targets)])
    root_mean = jnp.sqrt(squares / DS + epsilon)
    inner_mean = (squares / (root_mean * root_mean) - products / root_mean) / DS
    for half, (total, target) in enumerate(zip(totals, targets)):
        rows = slice(half * size, (half + 1) * size)
        normed = total / root_mean
        upstream = normed - target
        value = (upstream - normed * inner_mean) / root_mean
        slope_ref[rows, :] = value.reshape(-1, LANES).astype(jnp.bfloat16)
        grad_ref[rows, :] = (target - normed).reshape(-1, LANES)


def rows_kernel(lines_ref, out_ref):
    count, width = out_ref.shape
    depth = width // LANES // 2
    for t in range(2 * depth):
        base = t // depth * count * depth + t % depth
        tile = lines_ref[pl.ds(base, count, stride=depth), :]
        out_ref[:, t * LANES : (t + 1) * LANES] = tile.astype(jnp.bfloat16)


def rest_lines_kernel(*refs):
    units, outs = refs[:-2], refs[-2:]
    size = units[0].shape[0] // 2
    for half, out in enumerate(outs):
        for m, source in enumerate(units):
            out[m * size : (m + 1) * size, :] = source[half * size : (half + 1) * size]


def join_kernel(half, head_ref, rest_ref, out_ref, lines):
    size = head_ref.shape[0] // 2
    count, width = out_ref.shape
    depth = width // LANES
    lines[:size] = head_ref[half * size : (half + 1) * size].astype(jnp.float32)
    lines[size:] = rest_ref[...].astype(jnp.float32)
    for t in range(depth):
        tile = lines[pl.ds(t, count, stride=depth), :]
        out_ref[:, t * LANES : (t + 1) * LANES] = tile.astype(jnp.bfloat16)


def turn_kernel(own_ref, other_ref, out_ref):
    half = own_ref.shape[0]
    for i, source in enumerate((own_ref, other_ref)):
        out_ref[:, i * half : (i + 1) * half] = source[...].astype(jnp.float32).T.astype(
            jnp.bfloat16
        )


def grad_kernel(scale, step, per, states_ref, *refs):
    slopes, (out_ref, rhs, staged, sems) = refs[:-4], refs[-4:]
    copies, first = [], 0
    for chunk in range(len(slopes) // per):
        pieces = slopes[chunk * per : (chunk + 1) * per]
        count, width = pieces[0].shape
        for start in range(0, width, step):
            j = first // step
            for i, piece in enumerate(pieces):
                rhs[j % 2, i * count : (i + 1) * count, :] = piece[:, start : start + step]
            part = jnp.dot(states_ref[...], rhs[j % 2], preferred_element_type=jnp.float32)
            staged[j] = (part * scale).astype(jnp.bfloat16)
            copies.append(
                pltpu.make_async_copy(staged.at[j], out_ref.at[:, pl.ds(first, step)], sems.at[j])
            )
            copies[-1].start()
            first += step
    for copy in copies:
        copy.wait()


def grad_call(scale, states, slopes, per, shape, step=512):
    block_teacher, rows = states.shape
    count = shape[1] // step
    return pl.pallas_call(
        functools.partial(grad_kernel, scale, step, per),
        out_shape=jax.ShapeDtypeStruct(shape, jnp.bfloat16),
        in_specs=[IN_VMEM] * (len(slopes) + 1),
        out_specs=ANYWHERE,
        scratch_shapes=[
            pltpu.VMEM((2, rows, step), jnp.bfloat16),
            pltpu.VMEM((count, block_teacher, step), jnp.bfloat16),
            pltpu.SemaphoreType.DMA((count,)),
        ],
        compiler_params=pltpu.CompilerParams(vmem_limit_bytes=16 * MIB),
        cost_estimate=pl.CostEstimate(
            flops=2 * rows * block_teacher * shape[1],
            bytes_accessed=2 * block_teacher * shape[1],
            transcendentals=0,
        ),
    )(states, *slopes)


def far_across(values):
    arrived = []
    for m in range(1, len(values)):
        arrived.append(across(values[m], 0, path(0, 0, m)))
    return arrived


def line_shards(teacher, owner, proj_tiles, student_tiles):
    unit, _ = teacher.shape
    block_teacher, block_student = proj_tiles.shape
    near, far = NEAR, FEAT_SPLIT // NEAR
    half = FEAT_SPLIT * unit
    cut = block_student // 2
    depth = cut // LANES
    size = 2 * unit * depth
    bf16, f32 = jnp.bfloat16, jnp.float32

    place = [path(c, n, m) for c in range(2) for n in range(2) for m in range(far)]

    rows = (near * unit, block_teacher)
    packed = local_call(
        split_kernel,
        [((far * unit, block_teacher), bf16)] * near,
        [pltpu.with_memory_space_constraint(teacher, pltpu.HBM)],
        specs=[IN_HBM],
        scratch=[
            pltpu.VMEM(teacher.shape, bf16),
            pltpu.VMEM((near, far * unit, block_teacher), f32),
            pltpu.SemaphoreType.DMA((4,)),
        ],
    )
    slots = [packed[0]]
    for k in range(1, near):
        slots.append(across(packed[k], 0, k))
    held = local_call(
        functools.partial(far_kernel, near),
        [(rows, bf16)] * far,
        slots,
        scratch=[
            pltpu.VMEM((near, far * unit, block_teacher), f32),
            pltpu.VMEM((far, *rows), f32),
        ],
    )
    held = [held[0]] + far_across(held)

    tiles = pltpu.with_memory_space_constraint(proj_tiles, pltpu.HBM)
    part = (block_teacher, block_student // 2)
    work = dict(flops=block_teacher * half * block_student, moved=block_teacher * block_student)
    pick, first_tiles = local_call(
        functools.partial(first_kernel, place, unit),
        [((half, half), bf16), (part, bf16)],
        [pltpu.with_memory_space_constraint(owner, pltpu.HBM), tiles],
        specs=[IN_HBM] * 2,
        scratch=[
            pltpu.SMEM(owner.shape, owner.dtype),
            pltpu.SemaphoreType.DMA,
            pltpu.SemaphoreType.DMA((8,)),
        ],
        **work,
    )
    (second_tiles,) = local_call(
        functools.partial(second_kernel, part[1]),
        [(part, bf16)],
        [tiles],
        specs=[IN_HBM],
        scratch=[pltpu.SemaphoreType.DMA((8,))],
        **work,
    )
    halves = [((half // 2, cut), bf16), ((half // 2, cut), f32)]
    states, leaving, kept = local_call(
        order_kernel,
        [((half, block_teacher), bf16), *halves],
        [pick, *held, first_tiles],
        scratch=[pltpu.VMEM((half, block_teacher), bf16)],
        **work,
    )
    swapped = across(leaving, 0, 1)
    leaving, kept_b = local_call(rest_kernel, halves, [states, second_tiles], **work)
    swapped_b = across(leaving, 0, 1)
    small = size // 2
    leaving, staying = local_call(
        halve_kernel, [((half // 4, cut), bf16), ((half // 4, cut), f32)], [kept, swapped]
    )
    arrived = across(leaving, 0, path(0, 1, 0))
    own, *leaving = local_call(
        far_first_kernel,
        [((size, LANES), f32)] + [((size, LANES), bf16)] * (far - 1),
        [kept_b, swapped_b],
        scratch=[pltpu.VMEM((half // 2 * depth, LANES), f32)],
    )
    far_b = far_across([own, *leaving])
    own_a, *leaving = local_call(
        units_kernel,
        [((small, LANES), f32)] + [((small, LANES), bf16)] * (far - 1),
        [staying, arrived],
        scratch=[pltpu.VMEM((half // 4 * depth, LANES), f32)],
    )
    far_a = far_across([own_a, *leaving])
    leaving, own_b = local_call(
        far_sum_kernel, [((small, LANES), bf16), ((small, LANES), f32)], [own, *far_b]
    )
    near_b = across(leaving, 0, path(0, 1, 0))
    (target,) = local_call(target_kernel, [((size, LANES), f32)], [student_tiles])
    other_states = across(states, 1, 0)
    slope, grad = local_call(
        functools.partial(slope_kernel, unit),
        [((size, LANES), bf16), ((size, LANES), f32)],
        [own_a, *far_a, own_b, near_b, target],
    )
    (grad,) = local_call(rows_kernel, [((unit, block_student), bf16)], [grad])

    arrived = far_across([slope] * far)
    head_x = across(slope, 1, 1)
    head_y = across(slope, 0, 3)
    head_both = across(slope, 1, 2)
    rest_a, rest_b = local_call(
        rest_lines_kernel, [(((far - 1) * small, LANES), bf16)] * 2, arrived
    )

    def join(half_index, head, rest):
        (rows_of,) = local_call(
            functools.partial(join_kernel, half_index),
            [((far * unit, cut), bf16)],
            [head, rest],
            scratch=[pltpu.VMEM((far * small, LANES), f32)],
        )
        return rows_of

    scale = 1.0 / math.sqrt(lax.axis_size("group") * half)
    group_a = across(rest_a, 1, 1)
    near_b_rest = across(rest_b, 0, 3)
    group_b, near_a_rest = across(rest_b, 1, 1), across(rest_a, 0, 3)
    first, second = join(0, slope, rest_a), join(1, slope, rest_b)
    first_group, second_near = join(0, head_x, group_a), join(1, head_y, near_b_rest)
    second_group, first_near = join(1, head_x, group_b), join(0, head_y, near_a_rest)
    both_a = across(group_a, 0, 3)
    both_b = across(near_b_rest, 1, 1)
    first_both, second_both = join(0, head_both, both_a), join(1, head_both, both_b)
    (turned,) = local_call(turn_kernel, [((block_teacher, 2 * half), bf16)], [states, other_states])
    pieces = []
    for own, other in (
        ((first, first_near), (first_group, first_both)),
        ((second, second_near), (second_group, second_both)),
    ):
        pieces += [*own, *[across(piece, 0, 1) for piece in own]]
        pieces.append(across(other[0], 0, 1))
        pieces.append(across(other[1], 0, 1))
        pieces += other
    grad_proj = grad_call(scale, turned, pieces, len(pieces) // 2, (block_teacher, block_student))
    return grad_proj, grad


def shards(*blocks):
    if lax.axis_size("dev") == FEAT_SPLIT:
        return line_shards(*blocks)
    return wide_shards(*blocks)


def solution(mesh):
    placed = (P(("group", "dev"), None), P(), P("dev", None), P(("group", "dev"), None))
    return jax.shard_map(
        shards,
        mesh=mesh,
        in_specs=placed,
        out_specs=(P("dev", None), P(("group", "dev"), None)),
        check_vma=False,
    )
```
